16 devices in a mesh: dp: 2 (over y, z), tp: 8 (over x, core).
Axes of the slice: x: 4, y: 2, z: 1, core: 2. Of those that a mesh axis runs over, the one named last changes fastest.
The devices are a block of a 4x4x8 slice.
Arguments:
- x_in: bfloat16 [8192, 2048], P(('dp', 'tp')), parts along dimension 0
- dy_in: bfloat16 [8192, 2048], P(('dp', 'tp')), parts along dimension 0
- w_q: bfloat16 [2048, 8, 256], P(None, 'tp')
- w_k: bfloat16 [2048, 1, 256], replicated
- w_v: bfloat16 [2048, 1, 256], replicated
- w_o: bfloat16 [8, 256, 2048], P('tp')
Outputs:
- output 1: bfloat16 [8192, 2048], P(('dp', 'tp')), parts along dimension 0
- output 2: float32 [4096, 8, 256], P('dp', 'tp'), parts along dimension 0
- output 3: float32 [16, 256, 2048], P(('dp', 'tp')), parts along dimension 0
- output 4: float32 [4096, 256], P(('dp', 'tp')), parts along dimension 0
- output 5: float32 [4096, 256], P(('dp', 'tp')), parts along dimension 0
There are 2 independent parts. The reference program is written for one: setup_inputs(seed, part) draws one part's arguments, and reference() takes and returns one part's arrays. A program takes and returns all parts, laid end to end along the dimension named above; an argument that names none is the same for every part.
All inputs are finite; a program needn't handle non-finite values.
Results may differ from the reference program's by a relative error of at most 0.0101431.
Values are sent between devices in bfloat16 or wider.
A program may use at most 768 MiB of HBM per device.

```python
import jax
import jax.numpy as jnp
from jax import lax

D = 2048
HEADS = 8
KV_HEADS = 1
HEAD = 256
TOKENS = 4096
MODEL = 8

HEADS_DEV = HEADS // MODEL
REPL = MODEL // KV_HEADS
SCALE = HEAD ** -0.5


def setup_inputs(seed: int = 0, part: int = 0) -> dict:
    part_key = jax.random.fold_in(jax.random.key(seed), part)
    key_x, key_dy = jax.random.split(part_key)
    key_q, key_k, key_v, key_o = jax.random.split(jax.random.key(seed + 1), 4)
    fan_scale = D ** -0.5
    x_in = jax.random.normal(key_x, (TOKENS, D), jnp.float32).astype(jnp.bfloat16)
    dy_in = jax.random.normal(key_dy, (TOKENS, D), jnp.float32).astype(jnp.bfloat16)
    w_q = (jax.random.normal(key_q, (D, HEADS, HEAD), jnp.float32) * fan_scale).astype(jnp.bfloat16)
    w_k = (jax.random.normal(key_k, (D, KV_HEADS, HEAD), jnp.float32) * fan_scale).astype(jnp.bfloat16)
    w_v = (jax.random.normal(key_v, (D, KV_HEADS, HEAD), jnp.float32) * fan_scale).astype(jnp.bfloat16)
    w_o = (jax.random.normal(key_o, (HEADS, HEAD, D), jnp.float32) * fan_scale).astype(jnp.bfloat16)
    return dict(x_in=x_in, dy_in=dy_in, w_q=w_q, w_k=w_k, w_v=w_v, w_o=w_o)


def reference(x_in, dy_in, w_q, w_k, w_v, w_o):
    f32 = jnp.float32
    bf16 = jnp.bfloat16
    x_wide = x_in.astype(f32)
    dy_wide = dy_in.astype(f32)
    causal = lax.broadcasted_iota(jnp.int32, (TOKENS, TOKENS), 0) >= lax.broadcasted_iota(jnp.int32, (TOKENS, TOKENS), 1)
    wq_dev = jnp.transpose(w_q.reshape(D, MODEL, HEADS_DEV, HEAD), (1, 0, 2, 3))
    wo_dev = w_o.reshape(MODEL, HEADS_DEV, HEAD, D)
    wk_dev = jnp.repeat(jnp.transpose(w_k, (1, 0, 2)), REPL, axis=0)
    wv_dev = jnp.repeat(jnp.transpose(w_v, (1, 0, 2)), REPL, axis=0)

    def device_step(dx_acc, weights):
        wq_loc, wo_loc, wk_loc, wv_loc = weights
        wq_wide = wq_loc.astype(f32)
        wk_wide = wk_loc.astype(f32)
        wv_wide = wv_loc.astype(f32)
        queries = jnp.einsum("tc,che->hte", x_wide, wq_wide).astype(bf16)
        key_rows = jnp.dot(x_in, wk_loc, preferred_element_type=f32).astype(bf16)
        val_rows = jnp.dot(x_in, wv_loc, preferred_element_type=f32).astype(bf16)
        scores = jnp.einsum("hqe,ke->hqk", queries.astype(f32), key_rows.astype(f32)) * SCALE
        scores = jnp.where(causal, scores, -jnp.inf)
        attn_prob = jax.nn.softmax(scores, axis=-1)
        prob_bf = attn_prob.astype(bf16)
        attn_out = jnp.einsum("hqk,ke->hqe", prob_bf.astype(f32), val_rows.astype(f32)).astype(bf16)
        d_out = jnp.einsum("tc,hec->hte", dy_wide, wo_loc.astype(f32)).astype(bf16)
        grad_wo = jnp.einsum("hte,tc->hec", attn_out.astype(f32), dy_wide)
        d_prob = jnp.einsum("hqe,ke->hqk", d_out.astype(f32), val_rows.astype(f32))
        delta_row = jnp.sum(d_out.astype(f32) * attn_out.astype(f32), axis=-1, keepdims=True)
        d_score = (attn_prob * (d_prob - delta_row)).astype(bf16)
        d_query = (jnp.einsum("hqk,ke->hqe", d_score.astype(f32), key_rows.astype(f32)) * SCALE).astype(bf16)
        d_key = (jnp.einsum("hqk,hqe->ke", d_score.astype(f32), queries.astype(f32)) * SCALE).astype(bf16)
        d_val = jnp.einsum("hqk,hqe->ke", prob_bf.astype(f32), d_out.astype(f32)).astype(bf16)
        grad_wq = jnp.einsum("tc,hte->che", x_wide, d_query.astype(f32))
        dx_part = (jnp.einsum("hte,che->tc", d_query.astype(f32), wq_wide)
                   + jnp.dot(d_key.astype(f32), wk_wide.T)
                   + jnp.dot(d_val.astype(f32), wv_wide.T))
        return dx_acc + dx_part, (grad_wq, grad_wo, d_key, d_val)

    dx_sum, stacked = lax.scan(device_step, jnp.zeros((TOKENS, D), f32), (wq_dev, wo_dev, wk_dev, wv_dev))
    grad_wq, grad_wo, d_key, d_val = stacked
    dx_out = dx_sum.astype(bf16)
    dw_q = jnp.transpose(grad_wq, (1, 0, 2, 3)).reshape(D, HEADS, HEAD)
    dw_o = grad_wo.reshape(HEADS, HEAD, D)
    key_grp = d_key.reshape(KV_HEADS, REPL, TOKENS, HEAD).astype(f32)
    val_grp = d_val.reshape(KV_HEADS, REPL, TOKENS, HEAD).astype(f32)
    dw_k = jnp.einsum("tc,jrte->jce", x_wide, key_grp).reshape(KV_HEADS * D, HEAD)
    dw_v = jnp.einsum("tc,jrte->jce", x_wide, val_grp).reshape(KV_HEADS * D, HEAD)
    return dx_out, dw_q, dw_o, dw_k, dw_v
```

```python
import functools

import jax
import jax.numpy as jnp
from jax import lax
from jax.experimental import pallas as pl
from jax.experimental.pallas import tpu as pltpu
from jax.sharding import PartitionSpec as P

MESH = pl.DeviceIdType.MESH
F32 = jnp.float32
BF16 = jnp.bfloat16
LOG2E = 1.4426950408889634
VMEM_MAX = 67_043_328


def _mm(a, b):
    return lax.dot_general(a, b, (((1,), (0,)), ((), ())), preferred_element_type=F32)


def _mm_t(a, b):
    return lax.dot_general(a, b, (((1,), (1,)), ((), ())), preferred_element_type=F32)


def _ring(n):
    me = lax.axis_index("tp")
    core = lax.rem(me, 2)
    right = lax.rem(me + 2, n)
    left = lax.rem(me + n - 2, n)
    opp = lax.rem(me + n // 2, n)
    mate = me + 1 - 2 * core
    return me, core, right, left, opp, mate


def _barrier(devices):
    barrier = pltpu.get_barrier_semaphore()
    for d in devices:
        pl.semaphore_signal(barrier, inc=1, device_id={"tp": d}, device_id_type=MESH)
    pl.semaphore_wait(barrier, len(devices))


def _remote(src, dst, ssem, rsem, dev):
    return pltpu.make_async_remote_copy(
        src_ref=src, dst_ref=dst, send_sem=ssem, recv_sem=rsem,
        device_id={"tp": dev}, device_id_type=MESH)


def _gather_kernel(n, x, dy, wq, wk, wv, wo, xf, dyf, q, k, v, do,
                   buf, ssem_r, ssem_l, ssem_p, rsem, lsem, osem):
    me, core, right, left, opp, mate = _ring(n)
    rows = x.shape[0]
    half = rows // 2
    flip = 1 - 2 * core
    srcs, dsts = (x, dy), (xf, dyf)
    _barrier((left, right, mate))

    def view(a, blk, h):
        return dsts[a].at[blk, pl.ds(h * half, half)]

    def send(src, a, blk, h, ssem, dev):
        c = _remote(src, view(a, blk, h), ssem, rsem.at[a, blk * 2 + h], dev)
        c.start()
        sends.append(c)

    def recv(a, blk, h):
        _remote(view(a, blk, h), view(a, blk, h), ssem_p.at[a, 0],
                rsem.at[a, blk * 2 + h], mate).wait_recv()

    sends = []
    for a in range(2):
        for i, h in enumerate((0, 1)):
            own = srcs[a].at[pl.ds(h * half, half)]
            send(own, a, me, h, ssem_r.at[a, i], right)
            own = srcs[a].at[pl.ds((1 - h) * half, half)]
            send(own, a, me, 1 - h, ssem_l.at[a, i], left)
        for h in range(2):
            own = srcs[a].at[pl.ds(h * half, half)]
            send(own, a, me, h, ssem_p.at[a, h], mate)

    def project(a, b0, h0, b1, h1):
        def body(i, _):
            side, par = lax.rem(i, 2), i // 2
            blk = b0 + side * (b1 - b0) + par * flip
            h = h0 + side * (h1 - h0)
            pltpu.make_async_copy(view(a, blk, h), buf.at[i], lsem.at[i]).wait()
            at = pl.ds(pl.multiple_of(blk * rows + h * half, half), half)
            data = buf[i]
            if a == 0:
                q[at] = _mm(data, wq[...]).astype(BF16)
                k[at] = _mm(data, wk[...]).astype(BF16)
                v[at] = _mm(data, wv[...]).astype(BF16)
            else:
                do[at] = _mm_t(data, wo[...]).astype(BF16)
            return _
        lax.fori_loop(0, 4, body, 0)

    def first(a):
        for h in range(2):
            pltpu.make_async_copy(srcs[a].at[pl.ds(h * half, half)], buf.at[h], lsem.at[h]).start()
        for h in range(2):
            recv(a, mate, h)
            pltpu.make_async_copy(view(a, mate, h), buf.at[2 + h], lsem.at[2 + h]).start()
        project(a, me, 0, me, 1)
        outs = [pltpu.make_async_copy(buf.at[h], view(a, me, h), osem.at[h]) for h in range(2)]
        for c in outs:
            c.start()
        for c in outs:
            c.wait()

    def event(a, e):
        b0, h0, b1, h1 = ((left, 0, right, 1), (left, 1, right, 0), (opp, 0, opp, 1))[e - 1]
        recv(a, b0, h0)
        if e == 1:
            send(view(a, b0, h0), a, b0, h0, ssem_r.at[a, 2], right)
        send(view(a, b0, h0), a, b0, h0, ssem_p.at[a, 2 * e], mate)
        pltpu.make_async_copy(view(a, b0, h0), buf.at[0], lsem.at[0]).start()
        recv(a, b1, h1)
        if e == 1:
            send(view(a, b1, h1), a, b1, h1, ssem_l.at[a, 2], left)
        send(view(a, b1, h1), a, b1, h1, ssem_p.at[a, 2 * e + 1], mate)
        pltpu.make_async_copy(view(a, b1, h1), buf.at[1], lsem.at[1]).start()
        for i, (b, h) in enumerate(((b0, h0), (b1, h1))):
            recv(a, b + flip, h)
            pltpu.make_async_copy(view(a, b + flip, h), buf.at[2 + i], lsem.at[2 + i]).start()
        project(a, b0, h0, b1, h1)

    first(0)
    first(1)
    for a, e in ((0, 1), (0, 2), (1, 1), (1, 2), (0, 3), (1, 3)):
        event(a, e)
    for c in sends:
        c.wait_send()


def _grad_kernel(n, scale, q, k, v, do, xf, dyf, wq, wk, wv,
                 dx, dwq, dwo, dwk, dwv, wqf,
                 s_ref, p_ref, acc, lhs, dqs, dqr, kvr, kvx, dwr, dwx, xbuf,
                 mrow, lrow, oacc, qt, dot_,
                 w_sr, w_sl, w_sp, w_recv, dq_send, dq_recv, kv_send, kv_recv,
                 rs_send, rs_recv, x_sem, b_sem):
    me, core, right, left, opp, mate = _ring(n)
    chip = me // 2
    flip = 1 - 2 * core
    blk, width = q.shape[1], q.shape[2]
    model = dwq.shape[0]
    tile = model // (n // 2)
    lanes = 128
    whalf = model // 2
    _barrier([lax.rem(me + d, n) for d in range(1, n)])
    sends = []

    def wview(b, h):
        return wqf.at[b, pl.ds(h * whalf, whalf)]

    def wsend(src, b, h, ssem, dev):
        _remote(src, wview(b, h), ssem, w_recv.at[b * 2 + h], dev).start()

    def wrecv(b, h):
        _remote(wview(b, h), wview(b, h), w_sp.at[0], w_recv.at[b * 2 + h], mate).wait_recv()

    for i, h in enumerate((0, 1)):
        wsend(wq.at[pl.ds(h * whalf, whalf)], me, h, w_sr.at[i], right)
        wsend(wq.at[pl.ds((1 - h) * whalf, whalf)], me, 1 - h, w_sl.at[i], left)
    for h in range(2):
        wsend(wq.at[pl.ds(h * whalf, whalf)], me, h, w_sp.at[h], mate)

    def wevent(e):
        b0, h0, b1, h1 = ((left, 0, right, 1), (left, 1, right, 0), (opp, 0, opp, 1))[e - 1]
        wrecv(b0, h0)
        wrecv(b1, h1)
        if e == 1:
            wsend(wview(b0, h0), b0, h0, w_sr.at[2], right)
            wsend(wview(b1, h1), b1, h1, w_sl.at[2], left)
        wsend(wview(b0, h0), b0, h0, w_sp.at[2 * e], mate)
        wsend(wview(b1, h1), b1, h1, w_sp.at[2 * e + 1], mate)

    acc[...] = jnp.zeros_like(acc)
    dwo[...] = jnp.zeros_like(dwo)

    def fold(val, op):
        out = val[:, :lanes]
        for c in range(1, val.shape[1] // lanes):
            out = op(out, val[:, c * lanes:(c + 1) * lanes])
        return out

    def q_step(t, carry):
        nb = lax.rem(me + 1 + t, n)
        dy_copy = pltpu.make_async_copy(dyf.at[nb], xbuf.at[0], x_sem.at[0])
        dy_copy.start()
        qn = q[nb]
        don = do[nb]
        qt[...] = qn.T
        dot_[...] = don.T
        mrow[...] = jnp.full_like(mrow, -jnp.inf)

        def scores(j, _):
            sc = _mm_t(q[nb], k[j])
            s_ref[j] = sc
            mrow[...] = jnp.maximum(mrow[...], fold(sc, jnp.maximum))
            return _

        lax.fori_loop(0, nb, scores, 0)
        sc = _mm_t(qn, k[nb])
        keep = (lax.broadcasted_iota(jnp.int32, sc.shape, 0)
                >= lax.broadcasted_iota(jnp.int32, sc.shape, 1))
        sc = jnp.where(keep, sc, -jnp.inf)
        s_ref[nb] = sc
        m = jnp.max(jnp.maximum(mrow[...], fold(sc, jnp.maximum)), axis=1, keepdims=True)
        mrow[...] = jnp.broadcast_to(m, mrow.shape)
        lrow[...] = jnp.zeros_like(lrow)

        def expo(j, _):
            pr = jnp.exp2((s_ref[j] - mrow[:, :1]) * (scale * LOG2E))
            s_ref[j] = pr
            lrow[...] += fold(pr, jnp.add)
            return _

        lax.fori_loop(0, nb + 1, expo, 0)
        inv = 1.0 / jnp.sum(lrow[...], axis=1, keepdims=True)
        lrow[...] = jnp.broadcast_to(inv, lrow.shape)
        oacc[...] = jnp.zeros_like(oacc)

        def values(j, _):
            pb = (s_ref[j] * lrow[:, :1]).astype(BF16)
            p_ref[j] = pb
            oacc[...] += _mm(pb, v[j])
            return _

        lax.fori_loop(0, nb + 1, values, 0)
        ob = oacc[...].astype(BF16)
        delta = jnp.sum(don.astype(F32) * ob.astype(F32), axis=1, keepdims=True)
        mrow[...] = jnp.broadcast_to(delta, mrow.shape)
        oacc[...] = jnp.zeros_like(oacc)

        def grads(j, _):
            dp = _mm_t(do[nb], v[j])
            ds = (s_ref[j] * lrow[:, :1] * (dp - mrow[:, :1])).astype(BF16)
            oacc[...] += _mm(ds, k[j])
            acc[0, j] += _mm(qt[...], ds)
            acc[1, j] += _mm(dot_[...], p_ref[j])
            return _

        lax.fori_loop(0, nb + 1, grads, 0)
        dq = (oacc[...] * scale).astype(BF16)
        dqs[nb] = dq
        lhs[nb, 0:width] = dq.T

        @pl.when(t < n - 1)
        def _():
            _remote(dqs.at[nb], dqr.at[me], dq_send.at[nb], dq_recv.at[me], nb).start()

        @pl.when(t == n - 1)
        def _():
            dqr[me] = dq

        @pl.when(t == 3)
        def _():
            wevent(1)

        @pl.when(t == 5)
        def _():
            wevent(2)

        dy_copy.wait()
        ot = ob.T
        for c in range(model // tile):
            at = pl.ds(c * tile, tile)
            dwo[:, at] += _mm(ot, xbuf[0, :, at])
        return carry

    lax.fori_loop(0, n, q_step, 0)

    f_mine = jnp.where(core == 0, scale, 1.0).astype(F32)
    f_other = jnp.where(core == 0, 1.0, scale).astype(F32)

    def kv_copy(b):
        return _remote(p_ref.at[b, pl.ds(0, width)], lhs.at[b, pl.ds(2 * width, width)],
                       kv_send.at[b], kv_recv.at[b], mate)

    def convert(i, _):
        b = lax.rem(me - core + n // 2 + i, n)
        p_ref[b, 0:width] = (acc[1 - core, b] * f_other).astype(BF16)
        kv_copy(b).start()
        lhs[b, width:2 * width] = (acc[core, b] * f_mine).astype(BF16)
        return _

    lax.fori_loop(0, n, convert, 0)

    half_chips = n // 2

    def stag(b):
        return s_ref.at[half_chips + b // 2, pl.ds(lax.rem(b, 2) * width, width)]

    def pair(b):
        kv_copy(b).wait_recv()
        stag(b)[...] = (lhs[b, width:2 * width].astype(F32)
                        + lhs[b, 2 * width:3 * width].astype(F32))

    base = 2 * chip
    ob_, rb, lb = opp - core, right - core, left - core

    def rs_copy(src, dst, r, side, kind):
        return _remote(src, dst.at[side, kind], rs_send.at[r, side, kind],
                       rs_recv.at[r, side, kind], right if side == 0 else left)

    def rs_start(*args):
        c = rs_copy(*args)
        c.start()
        sends.append(c)

    def rs_wait(dst, r, side, kind):
        rs_copy(dst.at[side, kind], dst, r, side, kind).wait_recv()

    pair(ob_)
    rs_start(stag(ob_), kvr, 0, 0, 0)
    pair(ob_ + 1)
    rs_start(stag(ob_ + 1), kvr, 0, 1, 0)
    pair(rb + 1)
    rs_start(stag(rb + 1), kvr, 0, 0, 2)
    pair(lb)
    rs_start(stag(lb), kvr, 0, 1, 2)
    for b in (rb, lb + 1, base, base + 1):
        pair(b)

    def x_copy(b, slot):
        return pltpu.make_async_copy(xf.at[b], xbuf.at[slot], x_sem.at[slot])

    x_copy(0, 0).start()

    def x_step(b, carry):
        slot = lax.rem(b, 2)
        x_copy(b, slot).wait()

        @pl.when(b < n - 1)
        def _():
            x_copy(b + 1, 1 - slot).start()

        for c in range(model // tile):
            xt = xbuf[slot, :, c * tile:(c + 1) * tile]
            acc[0, c] += _mm(lhs[b, 0:width], xt)
            acc[1, c] += _mm(lhs[b, width:2 * width], xt) + _mm(lhs[b, 2 * width:3 * width], xt)
        return carry

    def clear(c, _):
        acc[0, c] = jnp.zeros_like(acc[0, c])
        acc[1, c] = jnp.zeros_like(acc[1, c])
        return _

    lax.fori_loop(0, half_chips, clear, 0)
    lax.fori_loop(0, n, x_step, 0)
    wevent(3)

    rs_wait(kvr, 0, 0, 0)
    stag(rb)[...] += kvr[0, 0]
    rs_start(stag(rb), kvr, 0, 0, 1)
    rs_wait(kvr, 0, 1, 0)
    stag(lb + 1)[...] += kvr[1, 0]
    rs_start(stag(lb + 1), kvr, 0, 1, 1)

    def part(b):
        return acc.at[1, b // 2, :, pl.ds(lax.rem(b, 2) * (tile // 2), tile // 2)]

    def part_cols(h):
        return slice(h * (tile // 2), (h + 1) * (tile // 2))

    rs_start(acc.at[1, ob_ // 2, :, pl.ds(0, tile // 2)], dwr, 1, 0, 0)
    rs_start(acc.at[1, ob_ // 2, :, pl.ds(tile // 2, tile // 2)], dwr, 1, 1, 0)
    rs_start(acc.at[1, rb // 2, :, pl.ds(tile // 2, tile // 2)], dwr, 1, 0, 2)
    rs_start(acc.at[1, lb // 2, :, pl.ds(0, tile // 2)], dwr, 1, 1, 2)

    for b in range(n):
        kv_copy(b).wait_send()
    for e, (b0, h0, b1, h1) in enumerate(((mate, 0, mate, 1), (left + flip, 0, right + flip, 1),
                                          (left + flip, 1, right + flip, 0), (opp + flip, 0, opp + flip, 1))):
        wrecv(b0, h0)
        wrecv(b1, h1)
    for d in range(1, n):
        peer = lax.rem(me + d, n)
        _remote(dqr.at[peer], dqr.at[peer], dq_send.at[peer], dq_recv.at[peer], peer).wait_recv()

    def w_copy(h, c, slot):
        return pltpu.make_async_copy(wqf.at[h, pl.ds(c * tile, tile)],
                                     p_ref.at[h, :, pl.ds(slot * width, width)], b_sem.at[slot, h])

    def own_copy(c, slot):
        return pltpu.make_async_copy(wq.at[pl.ds(c * tile, tile)],
                                     p_ref.at[me, :, pl.ds(slot * width, width)], b_sem.at[slot, me])

    def w_load(c, slot):
        own_copy(c, slot).start()
        for d in range(1, n):
            w_copy(lax.rem(me + d, n), c, slot).start()

    w_load(0, 0)
    for c in range(model // tile):
        slot = c % 2
        for h in range(n):
            w_copy(h, c, slot).wait()
        if c + 1 < model // tile:
            w_load(c + 1, 1 - slot)
        s_ref[c] = jnp.zeros_like(s_ref[c])

        def heads(h, _):
            s_ref[c] += _mm_t(dqr[h], p_ref[h, :, slot * width:(slot + 1) * width])
            return _

        lax.fori_loop(0, n, heads, 0)

    rs_wait(dwr, 1, 0, 0)
    acc[1, rb // 2, :, part_cols(0)] += dwr[0, 0]
    rs_start(acc.at[1, rb // 2, :, pl.ds(0, tile // 2)], dwr, 1, 0, 1)
    rs_wait(dwr, 1, 1, 0)
    acc[1, lb // 2, :, part_cols(1)] += dwr[1, 0]
    rs_start(acc.at[1, lb // 2, :, pl.ds(tile // 2, tile // 2)], dwr, 1, 1, 1)

    for c in range(model // tile):
        dwq[c * tile:(c + 1) * tile] = acc[0, c].T

    rs_wait(kvr, 0, 0, 1)
    rs_wait(kvr, 0, 1, 2)
    stag(base)[...] += kvr[0, 1] + kvr[1, 2]
    rs_wait(kvr, 0, 0, 2)
    rs_wait(kvr, 0, 1, 1)
    stag(base + 1)[...] += kvr[0, 2] + kvr[1, 1]
    swap = _remote(stag(mate), kvx.at[0], b_sem.at[2, 0], b_sem.at[2, 1], mate)
    swap.start()
    kvx[1] = stag(me)[...]
    swap.wait()
    kv_first = kvx[1 - core].T
    kv_second = kvx[core].T

    def split(val):
        hi = val.astype(BF16)
        rest = val - hi.astype(F32)
        mid = rest.astype(BF16)
        lo = (rest - mid.astype(F32)).astype(BF16)
        return hi, mid, lo

    for d in range(1, n):
        peer = lax.rem(me + d, n)
        _remote(dqr.at[peer], dqr.at[peer], dq_send.at[peer], dq_recv.at[peer], peer).wait_send()
    for i, parts in enumerate((split(kv_first), split(kv_second))):
        for g, val in enumerate(parts):
            dqs[3 * i + g] = val
    for c in range(model // tile):
        at = slice(c * tile, (c + 1) * tile)
        total = s_ref[c]
        for i, w in enumerate((wk, wv)):
            wt = w[at]
            total += (_mm_t(dqs[3 * i + 2], wt) + _mm_t(dqs[3 * i + 1], wt)) + _mm_t(dqs[3 * i], wt)
        dx[:, at] = total.astype(BF16)

    rs_wait(dwr, 1, 0, 1)
    rs_wait(dwr, 1, 1, 2)
    acc[1, base // 2, :, part_cols(0)] += dwr[0, 1] + dwr[1, 2]
    rs_wait(dwr, 1, 0, 2)
    rs_wait(dwr, 1, 1, 1)
    acc[1, base // 2, :, part_cols(1)] += dwr[0, 2] + dwr[1, 1]
    swap = _remote(part(mate), dwx.at[0], b_sem.at[2, 2], b_sem.at[2, 3], mate)
    swap.start()
    dwx[1] = part(me)[...]
    swap.wait()
    dwk[...] = dwx[1 - core].T
    dwv[...] = dwx[core].T

    for c in sends:
        c.wait_send()
    for i in range(3):
        _remote(wview(me, 0), wview(me, 0), w_sr.at[i], w_recv.at[0], mate).wait_send()
        _remote(wview(me, 0), wview(me, 0), w_sl.at[i], w_recv.at[0], mate).wait_send()
    for i in range(8):
        _remote(wview(me, 0), wview(me, 0), w_sp.at[i], w_recv.at[0], mate).wait_send()


def solution(mesh):
    n = mesh.shape["tp"]
    vmem = pl.BlockSpec(memory_space=pltpu.VMEM)
    hbm = pl.BlockSpec(memory_space=pl.ANY)
    dma = pltpu.SemaphoreType.DMA

    def local_grads(x_blk, dy_blk, wq_loc, w_k, w_v, wo_loc):
        model, kv_heads, width = w_k.shape
        rows = x_blk.shape[0]
        scale = width ** -0.5
        wq2 = wq_loc.reshape(model, width)
        wk2 = w_k.reshape(model, width)
        wv2 = w_v.reshape(model, width)
        wo2 = wo_loc.reshape(width, model)
        full = jax.ShapeDtypeStruct((n, rows, model), BF16)
        proj = jax.ShapeDtypeStruct((n * rows, width), BF16)
        xf, dyf, q, k, v, do = pl.pallas_call(
            functools.partial(_gather_kernel, n),
            name="gather_project",
            out_shape=(full, full, proj, proj, proj, proj),
            in_specs=[hbm, hbm, vmem, vmem, vmem, vmem],
            out_specs=(hbm, hbm, vmem, vmem, vmem, vmem),
            scratch_shapes=[
                pltpu.VMEM((4, rows // 2, model), BF16),
                dma((2, 3)), dma((2, 3)), dma((2, 8)), dma((2, 2 * n)), dma((4,)), dma((2,)),
            ],
            compiler_params=pltpu.CompilerParams(
                collective_id=0, has_side_effects=True, vmem_limit_bytes=32 * 2 ** 20),
        )(x_blk, dy_blk, wq2, wk2, wv2, wo2)
        q, k, v, do = (a.reshape(n, rows, width) for a in (q, k, v, do))
        tile = 2 * model // n
        dx, dwq, dwo, dwk, dwv, _ = pl.pallas_call(
            functools.partial(_grad_kernel, n, scale),
            name="attention_grads",
            out_shape=(
                jax.ShapeDtypeStruct((rows, model), BF16),
                jax.ShapeDtypeStruct((model, width), F32),
                jax.ShapeDtypeStruct((width, model), F32),
                jax.ShapeDtypeStruct((model // n, width), F32),
                jax.ShapeDtypeStruct((model // n, width), F32),
                jax.ShapeDtypeStruct((n, model, width), BF16),
            ),
            in_specs=[vmem] * 4 + [hbm] * 3 + [vmem] * 2,
            out_specs=(vmem,) * 5 + (hbm,),
            scratch_shapes=[
                pltpu.VMEM((n, rows, rows), F32),
                pltpu.VMEM((n, rows, rows), BF16),
                pltpu.VMEM((2, n, width, rows), F32),
                pltpu.VMEM((n, 3 * width, rows), BF16),
                pltpu.VMEM((n, rows, width), BF16),
                pltpu.VMEM((n, rows, width), BF16),
                pltpu.VMEM((2, 3, width, rows), F32),
                pltpu.VMEM((2, width, rows), F32),
                pltpu.VMEM((2, 3, width, tile // 2), F32),
                pltpu.VMEM((2, width, tile // 2), F32),
                pltpu.VMEM((2, rows, model), BF16),
                pltpu.VMEM((rows, 128), F32),
                pltpu.VMEM((rows, 128), F32),
                pltpu.VMEM((rows, width), F32),
                pltpu.VMEM((width, rows), BF16),
                pltpu.VMEM((width, rows), BF16),
                dma((3,)), dma((3,)), dma((8,)), dma((2 * n,)),
                dma((n,)), dma((n,)), dma((n,)), dma((n,)),
                dma((2, 2, 3)), dma((2, 2, 3)), dma((2,)), dma((3, n)),
            ],
            compiler_params=pltpu.CompilerParams(
                collective_id=1, has_side_effects=True, vmem_limit_bytes=VMEM_MAX),
        )(q, k, v, do, xf, dyf, wq2, wk2, wv2)
        return (dx, dwq.reshape(model, 1, width), dwo.reshape(1, width, model), dwk, dwv)

    tok_spec = P(("dp", "tp"))
    return jax.shard_map(
        local_grads,
        mesh=mesh,
        in_specs=(tok_spec, tok_spec, P(None, "tp", None), P(), P(), P("tp")),
        out_specs=(tok_spec, P("dp", "tp", None), tok_spec, tok_spec, tok_spec),
        check_vma=False,
    )
```

```python
import functools

import jax
import jax.numpy as jnp
from jax import lax
from jax.experimental import pallas as pl
from jax.experimental.pallas import tpu as pltpu
from jax.sharding import PartitionSpec as P

MESH = pl.DeviceIdType.MESH
F32 = jnp.float32
BF16 = jnp.bfloat16
LOG2E = 1.4426950408889634
VMEM_MAX = 67_043_328


def _mm(a, b):
    return lax.dot_general(a, b, (((1,), (0,)), ((), ())), preferred_element_type=F32)


def _mm_t(a, b):
    return lax.dot_general(a, b, (((1,), (1,)), ((), ())), preferred_element_type=F32)


def _ring(n):
    me = lax.axis_index("tp")
    core = lax.rem(me, 2)
    right = lax.rem(me + 2, n)
    left = lax.rem(me + n - 2, n)
    opp = lax.rem(me + n // 2, n)
    mate = me + 1 - 2 * core
    return me, core, right, left, opp, mate


def _barrier(devices):
    barrier = pltpu.get_barrier_semaphore()
    for d in devices:
        pl.semaphore_signal(barrier, inc=1, device_id={"tp": d}, device_id_type=MESH)
    pl.semaphore_wait(barrier, len(devices))


def _remote(src, dst, ssem, rsem, dev):
    return pltpu.make_async_remote_copy(
        src_ref=src, dst_ref=dst, send_sem=ssem, recv_sem=rsem,
        device_id={"tp": dev}, device_id_type=MESH)


def _kernel(n, scale, x, dy, wq, wk, wv, wo,
            dx, dwq, dwo, dwk, dwv, xf, dyf, wqf,
            q, k, v, do, wq_v, wk_v, wv_v, wo_v,
            s_ref, p_ref, acc, lhs, dqs, dqr, kvr, kvx, dwr, dwx, xbuf,
            mrow, lrow, oacc, qt, dot_, dwo_v, stage,
            g_sr, g_sl, g_sp, g_recv, l_sem,
            w_sr, w_sl, w_sp, w_recv, dq_send, dq_recv, kv_send, kv_recv,
            rs_send, rs_recv, x_sem, b_sem, o_sem):
    me, core, right, left, opp, mate = _ring(n)
    chip = me // 2
    flip = 1 - 2 * core
    blk, width = q.shape[1], q.shape[2]
    half = blk // 2
    model = x.shape[1]
    tile = model // (n // 2)
    lanes = 128
    whalf = model // 2
    _barrier([lax.rem(me + d, n) for d in range(1, n)])
    sends = []

    srcs, dsts = (x, dy), (xf, dyf)

    def view(a, b, h):
        return dsts[a].at[b, pl.ds(h * half, half)]

    def send(src, a, b, h, ssem, dev):
        _remote(src, view(a, b, h), ssem, g_recv.at[a, b * 2 + h], dev).start()

    def recv(a, b, h):
        _remote(view(a, b, h), view(a, b, h), g_sp.at[a, 0], g_recv.at[a, b * 2 + h], mate).wait_recv()

    def own(a, h):
        return srcs[a].at[pl.ds(h * half, half)]

    def send_own(a):
        for i, h in enumerate((0, 1)):
            send(own(a, h), a, me, h, g_sr.at[a, i], right)
            send(own(a, 1 - h), a, me, 1 - h, g_sl.at[a, i], left)

    def chunk(i):
        return xbuf.at[i // 2, pl.ds(lax.rem(i, 2) * half, half)]

    def load(src, i):
        return pltpu.make_async_copy(src, chunk(i), l_sem.at[i])

    def project(a, b0, h0, b1, h1):
        def body(i, carry):
            side, par = lax.rem(i, 2), i // 2
            b = b0 + side * (b1 - b0) + par * flip
            h = h0 + side * (h1 - h0)
            load(view(a, b, h), i).wait()
            at = pl.ds(pl.multiple_of(h * half, half), half)
            data = chunk(i)[...]
            if a == 0:
                q[b, at] = _mm(data, wq_v[...]).astype(BF16)
                k[b, at] = _mm(data, wk_v[...]).astype(BF16)
                v[b, at] = _mm(data, wv_v[...]).astype(BF16)
            else:
                do[b, at] = _mm_t(data, wo_v[...]).astype(BF16)
            return carry
        lax.fori_loop(0, 4, body, 0)

    def first(a):
        for h in range(2):
            load(own(a, h), h).start()
        for h in range(2):
            recv(a, mate, h)
            load(view(a, mate, h), 2 + h).start()
        project(a, me, 0, me, 1)

    def event(a, e):
        b0, h0, b1, h1 = ((left, 0, right, 1), (left, 1, right, 0), (opp, 0, opp, 1))[e - 1]
        for i, (b, h) in enumerate(((b0, h0), (b1, h1))):
            recv(a, b, h)
            if e == 1:
                send(view(a, b, h), a, b, h, (g_sr, g_sl)[i].at[a, 2], (right, left)[i])
            send(view(a, b, h), a, b, h, g_sp.at[a, 2 * e + i], mate)
            load(view(a, b, h), i).start()
        if e == 1:
            if a == 0:
                send_own(1)
            else:
                send_wq()
        for i, (b, h) in enumerate(((b0, h0), (b1, h1))):
            recv(a, b + flip, h)
            load(view(a, b + flip, h), 2 + i).start()
        project(a, b0, h0, b1, h1)

    def wview(b, h):
        return wqf.at[b, pl.ds(h * whalf, whalf)]

    def wsend(src, b, h, ssem, dev):
        _remote(src, wview(b, h), ssem, w_recv.at[b * 2 + h], dev).start()

    def wrecv(b, h):
        _remote(wview(b, h), wview(b, h), w_sp.at[0], w_recv.at[b * 2 + h], mate).wait_recv()

    def wown(h):
        return wq.at[pl.ds(h * whalf, whalf)]

    def send_wq():
        for i, h in enumerate((0, 1)):
            wsend(wown(h), me, h, w_sr.at[i], right)
            wsend(wown(1 - h), me, 1 - h, w_sl.at[i], left)

    def wevent(e):
        b0, h0, b1, h1 = ((left, 0, right, 1), (left, 1, right, 0), (opp, 0, opp, 1))[e - 1]
        wrecv(b0, h0)
        wrecv(b1, h1)
        if e == 1:
            wsend(wview(b0, h0), b0, h0, w_sr.at[2], right)
            wsend(wview(b1, h1), b1, h1, w_sl.at[2], left)
        wsend(wview(b0, h0), b0, h0, w_sp.at[2 * e], mate)
        wsend(wview(b1, h1), b1, h1, w_sp.at[2 * e + 1], mate)

    send_own(0)
    for a in range(2):
        for h in range(2):
            send(own(a, h), a, me, h, g_sp.at[a, h], mate)
    for h in range(2):
        wsend(wown(h), me, h, w_sp.at[h], mate)
    loads = [pltpu.make_async_copy(src, dst, o_sem.at[i])
             for i, (src, dst) in enumerate(((wq, wq_v), (wk, wk_v), (wv, wv_v), (wo, wo_v)))]
    for c in loads:
        c.start()
    acc[...] = jnp.zeros_like(acc)
    dwo_v[...] = jnp.zeros_like(dwo_v)
    for c in loads:
        c.wait()
    first(0)
    for e in (1, 2, 3):
        event(0, e)

    def fold(val, op):
        out = val[:, :lanes]
        for c in range(1, val.shape[1] // lanes):
            out = op(out, val[:, c * lanes:(c + 1) * lanes])
        return out

    def q_step(t, carry):
        p = t // 2
        nb = lax.rem(me + 2 * p + 2 * (p // 2) * (1 - 2 * lax.rem(p, 2)), n) + lax.rem(t, 2) * flip

        @pl.when(t == 0)
        def _():
            first(1)

        @pl.when(t == 2)
        def _():
            event(1, 1)
            event(1, 2)

        @pl.when(t == 6)
        def _():
            event(1, 3)

        @pl.when(t == 7)
        def _():
            wevent(1)

        dy_copy = pltpu.make_async_copy(dyf.at[nb], xbuf.at[0], x_sem.at[0])

        @pl.when(t == 0)
        def _():
            pltpu.make_async_copy(dy, xbuf.at[0], x_sem.at[0]).start()

        @pl.when(t > 0)
        def _():
            dy_copy.start()

        qn = q[nb]
        don = do[nb]
        qt[...] = qn.T
        dot_[...] = don.T
        mrow[...] = jnp.full_like(mrow, -jnp.inf)

        def scores(j, _):
            sc = _mm_t(q[nb], k[j])
            s_ref[j] = sc
            mrow[...] = jnp.maximum(mrow[...], fold(sc, jnp.maximum))
            return _

        lax.fori_loop(0, nb, scores, 0)
        sc = _mm_t(qn, k[nb])
        keep = (lax.broadcasted_iota(jnp.int32, sc.shape, 0)
                >= lax.broadcasted_iota(jnp.int32, sc.shape, 1))
        sc = jnp.where(keep, sc, -jnp.inf)
        s_ref[nb] = sc
        m = jnp.max(jnp.maximum(mrow[...], fold(sc, jnp.maximum)), axis=1, keepdims=True)
        mrow[...] = jnp.broadcast_to(m, mrow.shape)
        lrow[...] = jnp.zeros_like(lrow)

        def expo(j, _):
            pr = jnp.exp2((s_ref[j] - mrow[:, :1]) * (scale * LOG2E))
            s_ref[j] = pr
            lrow[...] += fold(pr, jnp.add)
            return _

        lax.fori_loop(0, nb + 1, expo, 0)
        inv = 1.0 / jnp.sum(lrow[...], axis=1, keepdims=True)
        lrow[...] = jnp.broadcast_to(inv, lrow.shape)
        oacc[...] = jnp.zeros_like(oacc)

        def values(j, _):
            pb = (s_ref[j] * lrow[:, :1]).astype(BF16)
            p_ref[j] = pb
            oacc[...] += _mm(pb, v[j])
            return _

        lax.fori_loop(0, nb + 1, values, 0)
        ob = oacc[...].astype(BF16)
        delta = jnp.sum(don.astype(F32) * ob.astype(F32), axis=1, keepdims=True)
        mrow[...] = jnp.broadcast_to(delta, mrow.shape)
        oacc[...] = jnp.zeros_like(oacc)

        def grads(j, _):
            dp = _mm_t(do[nb], v[j])
            ds = (s_ref[j] * lrow[:, :1] * (dp - mrow[:, :1])).astype(BF16)
            oacc[...] += _mm(ds, k[j])
            acc[0, j] += _mm(qt[...], ds)
            acc[1, j] += _mm(dot_[...], p_ref[j])
            return _

        lax.fori_loop(0, nb + 1, grads, 0)
        dq = (oacc[...] * scale).astype(BF16)
        dqs[nb] = dq
        lhs[nb, 0:width] = dq.T

        @pl.when(t > 0)
        def _():
            _remote(dqs.at[nb], dqr.at[me], dq_send.at[nb], dq_recv.at[me], nb).start()

        @pl.when(t == 0)
        def _():
            dqr[me] = dq

        dy_copy.wait()
        ot = ob.T
        for c in range(model // tile):
            at = pl.ds(c * tile, tile)
            dwo_v[:, at] += _mm(ot, xbuf[0, :, at])
        return carry

    lax.fori_loop(0, n, q_step, 0)

    f_mine = jnp.where(core == 0, scale, 1.0).astype(F32)
    f_other = jnp.where(core == 0, 1.0, scale).astype(F32)

    def kv_copy(b):
        return _remote(p_ref.at[b, pl.ds(0, width)], lhs.at[b, pl.ds(2 * width, width)],
                       kv_send.at[b], kv_recv.at[b], mate)

    def convert(i, _):
        b = lax.rem(me - core + n // 2 + i, n)
        p_ref[b, 0:width] = (acc[1 - core, b] * f_other).astype(BF16)
        kv_copy(b).start()
        lhs[b, width:2 * width] = (acc[core, b] * f_mine).astype(BF16)
        return _

    lax.fori_loop(0, n, convert, 0)

    out_wo = pltpu.make_async_copy(dwo_v, dwo, o_sem.at[0])
    out_wo.start()
    half_chips = n // 2

    def stag(b):
        return s_ref.at[half_chips + b // 2, pl.ds(lax.rem(b, 2) * width, width)]

    def pair(b):
        kv_copy(b).wait_recv()
        stag(b)[...] = (lhs[b, width:2 * width].astype(F32)
                        + lhs[b, 2 * width:3 * width].astype(F32))

    base = 2 * chip
    ob_, rb, lb = opp - core, right - core, left - core

    def rs_copy(src, dst, r, side, kind):
        return _remote(src, dst.at[side, kind], rs_send.at[r, side, kind],
                       rs_recv.at[r, side, kind], right if side == 0 else left)

    def rs_start(*args):
        c = rs_copy(*args)
        c.start()
        sends.append(c)

    def rs_wait(dst, r, side, kind):
        rs_copy(dst.at[side, kind], dst, r, side, kind).wait_recv()

    pair(ob_)
    rs_start(stag(ob_), kvr, 0, 0, 0)
    pair(ob_ + 1)
    rs_start(stag(ob_ + 1), kvr, 0, 1, 0)
    pair(rb + 1)
    rs_start(stag(rb + 1), kvr, 0, 0, 2)
    pair(lb)
    rs_start(stag(lb), kvr, 0, 1, 2)
    for b in (rb, lb + 1, base, base + 1):
        pair(b)

    def x_copy(b, slot):
        return pltpu.make_async_copy(xf.at[b], xbuf.at[slot], x_sem.at[slot])

    pltpu.make_async_copy(x, xbuf.at[0], x_sem.at[0]).start()
    wevent(2)

    def x_step(i, carry):
        slot = lax.rem(i, 2)
        b = lax.rem(me + i, n)
        x_copy(b, slot).wait()

        @pl.when(i < n - 1)
        def _():
            x_copy(lax.rem(me + i + 1, n), 1 - slot).start()

        for c in range(model // tile):
            xt = xbuf[slot, :, c * tile:(c + 1) * tile]
            acc[0, c] += _mm(lhs[b, 0:width], xt)
            acc[1, c] += _mm(lhs[b, width:2 * width], xt) + _mm(lhs[b, 2 * width:3 * width], xt)
        return carry

    def clear(c, _):
        acc[0, c] = jnp.zeros_like(acc[0, c])
        acc[1, c] = jnp.zeros_like(acc[1, c])
        return _

    lax.fori_loop(0, half_chips, clear, 0)
    lax.fori_loop(0, n, x_step, 0)
    wevent(3)

    rs_wait(kvr, 0, 0, 0)
    stag(rb)[...] += kvr[0, 0]
    rs_start(stag(rb), kvr, 0, 0, 1)
    rs_wait(kvr, 0, 1, 0)
    stag(lb + 1)[...] += kvr[1, 0]
    rs_start(stag(lb + 1), kvr, 0, 1, 1)

    def part(b):
        return acc.at[1, b // 2, :, pl.ds(lax.rem(b, 2) * (tile // 2), tile // 2)]

    def part_cols(h):
        return slice(h * (tile // 2), (h + 1) * (tile // 2))

    rs_start(acc.at[1, ob_ // 2, :, pl.ds(0, tile // 2)], dwr, 1, 0, 0)
    rs_start(acc.at[1, ob_ // 2, :, pl.ds(tile // 2, tile // 2)], dwr, 1, 1, 0)
    rs_start(acc.at[1, rb // 2, :, pl.ds(tile // 2, tile // 2)], dwr, 1, 0, 2)
    rs_start(acc.at[1, lb // 2, :, pl.ds(0, tile // 2)], dwr, 1, 1, 2)

    for b in range(n):
        kv_copy(b).wait_send()
    for e, (b0, h0, b1, h1) in enumerate(((mate, 0, mate, 1), (left + flip, 0, right + flip, 1),
                                          (left + flip, 1, right + flip, 0), (opp + flip, 0, opp + flip, 1))):
        wrecv(b0, h0)
        wrecv(b1, h1)
    for d in range(1, n):
        peer = lax.rem(me + d, n)
        _remote(dqr.at[peer], dqr.at[peer], dq_send.at[peer], dq_recv.at[peer], peer).wait_recv()

    def w_copy(h, c, slot):
        return pltpu.make_async_copy(wqf.at[h, pl.ds(c * tile, tile)],
                                     p_ref.at[h, :, pl.ds(slot * width, width)], b_sem.at[slot, h])

    def own_copy(c, slot):
        return pltpu.make_async_copy(wq.at[pl.ds(c * tile, tile)],
                                     p_ref.at[me, :, pl.ds(slot * width, width)], b_sem.at[slot, me])

    def w_load(c, slot):
        own_copy(c, slot).start()
        for d in range(1, n):
            w_copy(lax.rem(me + d, n), c, slot).start()

    w_load(0, 0)
    for c in range(model // tile):
        slot = c % 2
        for h in range(n):
            w_copy(h, c, slot).wait()
        if c + 1 < model // tile:
            w_load(c + 1, 1 - slot)
        s_ref[c] = jnp.zeros_like(s_ref[c])

        def heads(h, _):
            s_ref[c] += _mm_t(dqr[h], p_ref[h, :, slot * width:(slot + 1) * width])
            return _

        lax.fori_loop(0, n, heads, 0)

    rs_wait(dwr, 1, 0, 0)
    acc[1, rb // 2, :, part_cols(0)] += dwr[0, 0]
    rs_start(acc.at[1, rb // 2, :, pl.ds(0, tile // 2)], dwr, 1, 0, 1)
    rs_wait(dwr, 1, 1, 0)
    acc[1, lb // 2, :, part_cols(1)] += dwr[1, 0]
    rs_start(acc.at[1, lb // 2, :, pl.ds(tile // 2, tile // 2)], dwr, 1, 1, 1)

    for c in range(model // tile):
        for g in range(2):
            stage[c, pl.ds(g, tile, stride=2)] = acc[0, c, g * lanes:(g + 1) * lanes].T
        pltpu.make_async_copy(stage.at[c], dwq.at[pl.ds(c * 2 * tile, 2 * tile)], l_sem.at[c]).start()

    rs_wait(kvr, 0, 0, 1)
    rs_wait(kvr, 0, 1, 2)
    stag(base)[...] += kvr[0, 1] + kvr[1, 2]
    rs_wait(kvr, 0, 0, 2)
    rs_wait(kvr, 0, 1, 1)
    stag(base + 1)[...] += kvr[0, 2] + kvr[1, 1]
    swap = _remote(stag(mate), kvx.at[0], b_sem.at[2, 0], b_sem.at[2, 1], mate)
    swap.start()
    kvx[1] = stag(me)[...]
    swap.wait()
    kv_first = kvx[1 - core].T
    kv_second = kvx[core].T

    def split(val):
        hi = val.astype(BF16)
        rest = val - hi.astype(F32)
        mid = rest.astype(BF16)
        lo = (rest - mid.astype(F32)).astype(BF16)
        return hi, mid, lo

    for d in range(1, n):
        peer = lax.rem(me + d, n)
        _remote(dqr.at[peer], dqr.at[peer], dq_send.at[peer], dq_recv.at[peer], peer).wait_send()
    for i, parts in enumerate((split(kv_first), split(kv_second))):
        for g, val in enumerate(parts):
            dqs[3 * i + g] = val
    for c in range(model // tile):
        at = slice(c * tile, (c + 1) * tile)
        total = s_ref[c]
        for i, w in enumerate((wk_v, wv_v)):
            wt = w[at]
            total += (_mm_t(dqs[3 * i + 2], wt) + _mm_t(dqs[3 * i + 1], wt)) + _mm_t(dqs[3 * i], wt)
        xbuf[0, :, at] = total.astype(BF16)
    out_dx = pltpu.make_async_copy(xbuf.at[0], dx, x_sem.at[0])
    out_dx.start()

    outs = [out_wo, out_dx]
    rs_wait(dwr, 1, 0, 1)
    rs_wait(dwr, 1, 1, 2)
    acc[1, base // 2, :, part_cols(0)] += dwr[0, 1] + dwr[1, 2]
    rs_wait(dwr, 1, 0, 2)
    rs_wait(dwr, 1, 1, 1)
    acc[1, base // 2, :, part_cols(1)] += dwr[0, 2] + dwr[1, 1]
    swap = _remote(part(mate), dwx.at[0], b_sem.at[2, 2], b_sem.at[2, 3], mate)
    swap.start()
    dwx[1] = part(me)[...]
    swap.wait()
    for i, (val, out) in enumerate(((dwx[1 - core].T, dwk), (dwx[core].T, dwv))):
        oacc[i * width:(i + 1) * width] = val
        outs.append(pltpu.make_async_copy(oacc.at[pl.ds(i * width, width)], out, o_sem.at[1 + i]))
        outs[-1].start()
    for c in outs:
        c.wait()
    for c in range(model // tile):
        pltpu.make_async_copy(stage.at[c], dwq.at[pl.ds(c * 2 * tile, 2 * tile)], l_sem.at[c]).wait()

    for c in sends:
        c.wait_send()
    for a in range(2):
        for i in range(3):
            _remote(view(a, me, 0), view(a, me, 0), g_sr.at[a, i], g_recv.at[a, 0], mate).wait_send()
            _remote(view(a, me, 0), view(a, me, 0), g_sl.at[a, i], g_recv.at[a, 0], mate).wait_send()
        for i in range(8):
            _remote(view(a, me, 0), view(a, me, 0), g_sp.at[a, i], g_recv.at[a, 0], mate).wait_send()
    for i in range(3):
        _remote(wview(me, 0), wview(me, 0), w_sr.at[i], w_recv.at[0], mate).wait_send()
        _remote(wview(me, 0), wview(me, 0), w_sl.at[i], w_recv.at[0], mate).wait_send()
    for i in range(8):
        _remote(wview(me, 0), wview(me, 0), w_sp.at[i], w_recv.at[0], mate).wait_send()


def solution(mesh):
    n = mesh.shape["tp"]
    hbm = pl.BlockSpec(memory_space=pl.ANY)
    dma = pltpu.SemaphoreType.DMA

    def local_grads(x_blk, dy_blk, wq_loc, w_k, w_v, wo_loc):
        model, kv_heads, width = w_k.shape
        rows = x_blk.shape[0]
        scale = width ** -0.5
        wq2 = wq_loc.reshape(model, width)
        wk2 = w_k.reshape(model, width)
        wv2 = w_v.reshape(model, width)
        wo2 = wo_loc.reshape(width, model)
        tile = 2 * model // n
        full = jax.ShapeDtypeStruct((n, rows, model), BF16)
        proj = pltpu.VMEM((n, rows, width), BF16)
        dx, dwq, dwo, dwk, dwv, _, _, _ = pl.pallas_call(
            functools.partial(_kernel, n, scale),
            name="attention_grads",
            out_shape=(
                jax.ShapeDtypeStruct((rows, model), BF16),
                jax.ShapeDtypeStruct((2 * model, 128), F32),
                jax.ShapeDtypeStruct((width, model), F32),
                jax.ShapeDtypeStruct((model // n, width), F32),
                jax.ShapeDtypeStruct((model // n, width), F32),
                full, full,
                jax.ShapeDtypeStruct((n, model, width), BF16),
            ),
            in_specs=[hbm] * 6,
            out_specs=(hbm,) * 8,
            scratch_shapes=[
                proj, proj, proj, proj,
                pltpu.VMEM((model, width), BF16),
                pltpu.VMEM((model, width), BF16),
                pltpu.VMEM((model, width), BF16),
                pltpu.VMEM((width, model), BF16),
                pltpu.VMEM((n, rows, rows), F32),
                pltpu.VMEM((n, rows, rows), BF16),
                pltpu.VMEM((2, n, width, rows), F32),
                pltpu.VMEM((n, 3 * width, rows), BF16),
                pltpu.VMEM((n, rows, width), BF16),
                pltpu.VMEM((n, rows, width), BF16),
                pltpu.VMEM((2, 3, width, rows), F32),
                pltpu.VMEM((2, width, rows), F32),
                pltpu.VMEM((2, 3, width, tile // 2), F32),
                pltpu.VMEM((2, width, tile // 2), F32),
                pltpu.VMEM((2, rows, model), BF16),
                pltpu.VMEM((rows, 128), F32),
                pltpu.VMEM((rows, 128), F32),
                pltpu.VMEM((rows, width), F32),
                pltpu.VMEM((width, rows), BF16),
                pltpu.VMEM((width, rows), BF16),
                pltpu.VMEM((width, model), F32),
                pltpu.VMEM((n // 2, 2 * tile, 128), F32),
                dma((2, 3)), dma((2, 3)), dma((2, 8)), dma((2, 2 * n)), dma((4,)),
                dma((3,)), dma((3,)), dma((8,)), dma((2 * n,)),
                dma((n,)), dma((n,)), dma((n,)), dma((n,)),
                dma((2, 2, 3)), dma((2, 2, 3)), dma((2,)), dma((3, n)), dma((4,)),
            ],
            compiler_params=pltpu.CompilerParams(
                collective_id=0, has_side_effects=True, vmem_limit_bytes=VMEM_MAX),
        )(x_blk, dy_blk, wq2, wk2, wv2, wo2)
        return (dx, dwq.reshape(model, 1, width), dwo.reshape(1, width, model), dwk, dwv)

    tok_spec = P(("dp", "tp"))
    return jax.shard_map(
        local_grads,
        mesh=mesh,
        in_specs=(tok_spec, tok_spec, P(None, "tp", None), P(), P(), P("tp")),
        out_specs=(tok_spec, P("dp", "tp", None), tok_spec, tok_spec, tok_spec),
        check_vma=False,
    )
```

```python
import functools

import jax
import jax.numpy as jnp
from jax import lax
from jax.experimental import pallas as pl
from jax.experimental.pallas import tpu as pltpu
from jax.sharding import PartitionSpec as P

MESH = pl.DeviceIdType.MESH
F32 = jnp.float32
BF16 = jnp.bfloat16
LOG2E = 1.4426950408889634
VMEM_MAX = 67_043_328


def _mm(a, b):
    return lax.dot_general(a, b, (((1,), (0,)), ((), ())), preferred_element_type=F32)


def _mm_t(a, b):
    return lax.dot_general(a, b, (((1,), (1,)), ((), ())), preferred_element_type=F32)


def _ring(n):
    me = lax.axis_index("tp")
    core = lax.rem(me, 2)
    right = lax.rem(me + 2, n)
    left = lax.rem(me + n - 2, n)
    opp = lax.rem(me + n // 2, n)
    mate = me + 1 - 2 * core
    return me, core, right, left, opp, mate


def _barrier(devices):
    barrier = pltpu.get_barrier_semaphore()
    for d in devices:
        pl.semaphore_signal(barrier, inc=1, device_id={"tp": d}, device_id_type=MESH)
    pl.semaphore_wait(barrier, len(devices))


def _remote(src, dst, ssem, rsem, dev):
    return pltpu.make_async_remote_copy(
        src_ref=src, dst_ref=dst, send_sem=ssem, recv_sem=rsem,
        device_id={"tp": dev}, device_id_type=MESH)


def _kernel(n, scale, x, dy, wq, wk, wv, wo,
            dx, dwq, dwo, dwk, dwv, xf, dyf, wqf,
            q, k, v, do, wq_v, wk_v, wv_v, wo_v,
            s_ref, p_ref, acc, lhs, o, lse, dqr, kvr, kvx, dwr, dwx, xbuf,
            mrow, lrow, oacc, qt, dot_, dwo_v,
            g_sr, g_sl, g_sp, g_recv, l_sem,
            w_sr, w_sl, w_sp, w_recv, dq_send, dq_recv, kv_send, kv_recv,
            rs_send, rs_recv, x_sem, b_sem, o_sem):
    me, core, right, left, opp, mate = _ring(n)
    chip = me // 2
    flip = 1 - 2 * core
    blk, width = q.shape[1], q.shape[2]
    half = blk // 2
    model = x.shape[1]
    tile = model // (n // 2)
    lanes = 128
    whalf = model // 2
    _barrier([lax.rem(me + d, n) for d in range(1, n)])
    sends = []

    srcs, dsts = (x, dy), (xf, dyf)

    def view(a, b, h):
        return dsts[a].at[b, pl.ds(h * half, half)]

    def send(src, a, b, h, ssem, dev):
        _remote(src, view(a, b, h), ssem, g_recv.at[a, b * 2 + h], dev).start()

    def recv(a, b, h):
        _remote(view(a, b, h), view(a, b, h), g_sp.at[a, 0], g_recv.at[a, b * 2 + h], mate).wait_recv()

    def own(a, h):
        return srcs[a].at[pl.ds(h * half, half)]

    def send_own(a):
        for i, h in enumerate((0, 1)):
            send(own(a, h), a, me, h, g_sr.at[a, i], right)
            send(own(a, 1 - h), a, me, 1 - h, g_sl.at[a, i], left)

    def chunk(i):
        return xbuf.at[i // 2, pl.ds(lax.rem(i, 2) * half, half)]

    def load(src, i):
        return pltpu.make_async_copy(src, chunk(i), l_sem.at[i])

    def project(a, b0, h0, b1, h1):
        def body(i, carry):
            side, par = lax.rem(i, 2), i // 2
            b = b0 + side * (b1 - b0) + par * flip
            h = h0 + side * (h1 - h0)
            load(view(a, b, h), i).wait()
            at = pl.ds(pl.multiple_of(h * half, half), half)
            data = chunk(i)[...]
            if a == 0:
                q[b, at] = _mm(data, wq_v[...]).astype(BF16)
                k[b, at] = _mm(data, wk_v[...]).astype(BF16)
                v[b, at] = _mm(data, wv_v[...]).astype(BF16)
            else:
                do[b, at] = _mm_t(data, wo_v[...]).astype(BF16)
            return carry
        lax.fori_loop(0, 4, body, 0)

    def first(a):
        for h in range(2):
            load(own(a, h), h).start()
        for h in range(2):
            recv(a, mate, h)
            load(view(a, mate, h), 2 + h).start()
        project(a, me, 0, me, 1)

    def event(a, e):
        b0, h0, b1, h1 = ((left, 0, right, 1), (left, 1, right, 0), (opp, 0, opp, 1))[e - 1]
        for i, (b, h) in enumerate(((b0, h0), (b1, h1))):
            recv(a, b, h)
            if e == 1:
                send(view(a, b, h), a, b, h, (g_sr, g_sl)[i].at[a, 2], (right, left)[i])
            send(view(a, b, h), a, b, h, g_sp.at[a, 2 * e + i], mate)
            load(view(a, b, h), i).start()
        if e == 1:
            if a == 0:
                send_own(1)
            else:
                send_wq()
        for i, (b, h) in enumerate(((b0, h0), (b1, h1))):
            recv(a, b + flip, h)
            load(view(a, b + flip, h), 2 + i).start()
        project(a, b0, h0, b1, h1)

    def wview(b, h):
        return wqf.at[b, pl.ds(h * whalf, whalf)]

    def wsend(src, b, h, ssem, dev):
        _remote(src, wview(b, h), ssem, w_recv.at[b * 2 + h], dev).start()

    def wrecv(b, h):
        _remote(wview(b, h), wview(b, h), w_sp.at[0], w_recv.at[b * 2 + h], mate).wait_recv()

    def wown(h):
        return wq.at[pl.ds(h * whalf, whalf)]

    def send_wq():
        for i, h in enumerate((0, 1)):
            wsend(wown(h), me, h, w_sr.at[i], right)
            wsend(wown(1 - h), me, 1 - h, w_sl.at[i], left)

    def wevent(e):
        b0, h0, b1, h1 = ((left, 0, right, 1), (left, 1, right, 0), (opp, 0, opp, 1))[e - 1]
        wrecv(b0, h0)
        wrecv(b1, h1)
        if e == 1:
            wsend(wview(b0, h0), b0, h0, w_sr.at[2], right)
            wsend(wview(b1, h1), b1, h1, w_sl.at[2], left)
        wsend(wview(b0, h0), b0, h0, w_sp.at[2 * e], mate)
        wsend(wview(b1, h1), b1, h1, w_sp.at[2 * e + 1], mate)

    send_own(0)
    for a in range(2):
        for h in range(2):
            send(own(a, h), a, me, h, g_sp.at[a, h], mate)
    for h in range(2):
        wsend(wown(h), me, h, w_sp.at[h], mate)
    loads = [pltpu.make_async_copy(src, dst, o_sem.at[i])
             for i, (src, dst) in enumerate(((wq, wq_v), (wk, wk_v), (wv, wv_v), (wo, wo_v)))]
    for c in loads:
        c.start()
    acc[...] = jnp.zeros_like(acc)
    dwo_v[...] = jnp.zeros_like(dwo_v)
    for c in loads:
        c.wait()
    first(0)
    for e in (1, 2, 3):
        event(0, e)

    def fold(val, op):
        out = val[:, :lanes]
        for c in range(1, val.shape[1] // lanes):
            out = op(out, val[:, c * lanes:(c + 1) * lanes])
        return out

    def groups(val):
        return [val[:, c * lanes:(c + 1) * lanes] for c in range(val.shape[1] // lanes)]

    def expo(val, top):
        return jnp.exp2((val - top) * (scale * LOG2E))

    keep = (lax.broadcasted_iota(jnp.int32, (blk, blk), 0)
            >= lax.broadcasted_iota(jnp.int32, (blk, blk), 1))

    def forward(nb, carry):
        mrow[...] = jnp.full_like(mrow, jnp.finfo(F32).min)
        lrow[...] = jnp.zeros_like(lrow)

        def stats(j, sc):
            s_ref[j] = sc
            old = mrow[...]
            top = jnp.maximum(old, fold(sc, jnp.maximum))
            total = lrow[...] * expo(old, top)
            for part in groups(sc):
                total += expo(part, top)
            mrow[...] = top
            lrow[...] = total

        def scores(j, carry):
            stats(j, _mm_t(q[nb], k[j]))
            return carry

        lax.fori_loop(0, nb, scores, 0)
        stats(nb, jnp.where(keep, _mm_t(q[nb], k[nb]), -jnp.inf))
        top = jnp.max(mrow[...], axis=1, keepdims=True)
        total = jnp.sum(lrow[...] * expo(mrow[...], top), axis=1, keepdims=True)
        lse[nb] = jnp.broadcast_to(top + jnp.log(total) * (1.0 / scale), mrow.shape)
        oacc[...] = jnp.zeros_like(oacc)

        def values(j, carry):
            shift = lse[nb]
            pb = jnp.concatenate([expo(part, shift).astype(BF16) for part in groups(s_ref[j])], axis=1)
            oacc[...] += _mm(pb, v[j])
            return carry

        lax.fori_loop(0, nb + 1, values, 0)
        o[nb] = oacc[...].astype(BF16)
        return carry

    lax.fori_loop(0, n, forward, 0)

    def q_step(t, carry):
        p = t // 2
        nb = lax.rem(me + 2 * p + 2 * (p // 2) * (1 - 2 * lax.rem(p, 2)), n) + lax.rem(t, 2) * flip

        @pl.when(t == 0)
        def _():
            first(1)
            event(1, 1)

        @pl.when(t == 2)
        def _():
            event(1, 2)

        @pl.when(t == 6)
        def _():
            event(1, 3)

        @pl.when(t == 7)
        def _():
            wevent(1)

        dy_copy = pltpu.make_async_copy(dyf.at[nb], xbuf.at[0], x_sem.at[0])

        @pl.when(t == 0)
        def _():
            pltpu.make_async_copy(dy, xbuf.at[0], x_sem.at[0]).start()

        @pl.when(t > 0)
        def _():
            dy_copy.start()

        qt[...] = q[nb].T
        dot_[...] = do[nb].T
        delta = jnp.sum(do[nb].astype(F32) * o[nb].astype(F32), axis=1, keepdims=True)
        mrow[...] = jnp.broadcast_to(delta, mrow.shape)
        oacc[...] = jnp.zeros_like(oacc)

        def grads(j, mask):
            sc = groups(_mm_t(q[nb], k[j]))
            dp = groups(_mm_t(do[nb], v[j]))
            shift, less = lse[nb], mrow[...]
            pr = [expo(part, shift) for part in sc]
            if mask:
                pr = [jnp.where(kg, part, 0.0) for kg, part in zip(groups(keep), pr)]
            ds = jnp.concatenate([(pp * (dd - less)).astype(BF16) for pp, dd in zip(pr, dp)], axis=1)
            pb = jnp.concatenate([pp.astype(BF16) for pp in pr], axis=1)
            oacc[...] += _mm(ds, k[j])
            acc[0, j] += _mm(qt[...], ds)
            acc[1, j] += _mm(dot_[...], pb)

        def below(j, carry):
            grads(j, False)
            return carry

        lax.fori_loop(0, nb, below, 0)
        grads(nb, True)
        dq = (oacc[...] * scale).astype(BF16)
        q[nb] = dq
        lhs[nb, 0:width] = dq.T

        @pl.when(t > 0)
        def _():
            _remote(q.at[nb], dqr.at[me], dq_send.at[nb], dq_recv.at[me], nb).start()

        @pl.when(t == 0)
        def _():
            dqr[me] = dq

        dy_copy.wait()
        ot = o[nb].T
        for c in range(model // tile):
            at = pl.ds(c * tile, tile)
            dwo_v[:, at] += _mm(ot, xbuf[0, :, at])
        return carry

    lax.fori_loop(0, n, q_step, 0)

    f_mine = jnp.where(core == 0, scale, 1.0).astype(F32)
    f_other = jnp.where(core == 0, 1.0, scale).astype(F32)

    def kv_copy(b):
        return _remote(p_ref.at[b, pl.ds(0, width)], lhs.at[b, pl.ds(2 * width, width)],
                       kv_send.at[b], kv_recv.at[b], mate)

    def convert(i, _):
        b = lax.rem(me - core + n // 2 + i, n)
        p_ref[b, 0:width] = (acc[1 - core, b] * f_other).astype(BF16)
        kv_copy(b).start()
        lhs[b, width:2 * width] = (acc[core, b] * f_mine).astype(BF16)
        return _

    lax.fori_loop(0, n, convert, 0)

    out_wo = pltpu.make_async_copy(dwo_v, dwo, o_sem.at[0])
    out_wo.start()
    half_chips = n // 2

    def stag(b):
        return s_ref.at[half_chips + b // 2, pl.ds(lax.rem(b, 2) * width, width)]

    def pair(b):
        kv_copy(b).wait_recv()
        stag(b)[...] = (lhs[b, width:2 * width].astype(F32)
                        + lhs[b, 2 * width:3 * width].astype(F32))

    base = 2 * chip
    ob_, rb, lb = opp - core, right - core, left - core

    def rs_copy(src, dst, r, side, kind):
        return _remote(src, dst.at[side, kind], rs_send.at[r, side, kind],
                       rs_recv.at[r, side, kind], right if side == 0 else left)

    def rs_start(*args):
        c = rs_copy(*args)
        c.start()
        sends.append(c)

    def rs_wait(dst, r, side, kind):
        rs_copy(dst.at[side, kind], dst, r, side, kind).wait_recv()

    pair(ob_)
    rs_start(stag(ob_), kvr, 0, 0, 0)
    pair(ob_ + 1)
    rs_start(stag(ob_ + 1), kvr, 0, 1, 0)
    pair(rb + 1)
    rs_start(stag(rb + 1), kvr, 0, 0, 2)
    pair(lb)
    rs_start(stag(lb), kvr, 0, 1, 2)
    for b in (rb, lb + 1, base, base + 1):
        pair(b)

    def x_copy(b, slot):
        return pltpu.make_async_copy(xf.at[b], xbuf.at[slot], x_sem.at[slot])

    pltpu.make_async_copy(x, xbuf.at[0], x_sem.at[0]).start()
    wevent(2)

    def x_step(i, carry):
        slot = lax.rem(i, 2)
        b = lax.rem(me + i, n)
        x_copy(b, slot).wait()

        @pl.when(i < n - 1)
        def _():
            x_copy(lax.rem(me + i + 1, n), 1 - slot).start()

        for c in range(model // tile):
            xt = xbuf[slot, :, c * tile:(c + 1) * tile]
            acc[0, c] += _mm(lhs[b, 0:width], xt)
            acc[1, c] += _mm(lhs[b, width:2 * width], xt) + _mm(lhs[b, 2 * width:3 * width], xt)
        return carry

    def clear(c, _):
        acc[0, c] = jnp.zeros_like(acc[0, c])
        acc[1, c] = jnp.zeros_like(acc[1, c])
        return _

    lax.fori_loop(0, half_chips, clear, 0)
    lax.fori_loop(0, n, x_step, 0)
    wevent(3)

    rs_wait(kvr, 0, 0, 0)
    stag(rb)[...] += kvr[0, 0]
    rs_start(stag(rb), kvr, 0, 0, 1)
    rs_wait(kvr, 0, 1, 0)
    stag(lb + 1)[...] += kvr[1, 0]
    rs_start(stag(lb + 1), kvr, 0, 1, 1)

    def part(b):
        return acc.at[1, b // 2, :, pl.ds(lax.rem(b, 2) * (tile // 2), tile // 2)]

    def part_cols(h):
        return slice(h * (tile // 2), (h + 1) * (tile // 2))

    rs_start(acc.at[1, ob_ // 2, :, pl.ds(0, tile // 2)], dwr, 1, 0, 0)
    rs_start(acc.at[1, ob_ // 2, :, pl.ds(tile // 2, tile // 2)], dwr, 1, 1, 0)
    rs_start(acc.at[1, rb // 2, :, pl.ds(tile // 2, tile // 2)], dwr, 1, 0, 2)
    rs_start(acc.at[1, lb // 2, :, pl.ds(0, tile // 2)], dwr, 1, 1, 2)

    for b in range(n):
        kv_copy(b).wait_send()
    for e, (b0, h0, b1, h1) in enumerate(((mate, 0, mate, 1), (left + flip, 0, right + flip, 1),
                                          (left + flip, 1, right + flip, 0), (opp + flip, 0, opp + flip, 1))):
        wrecv(b0, h0)
        wrecv(b1, h1)
    for d in range(1, n):
        peer = lax.rem(me + d, n)
        _remote(dqr.at[peer], dqr.at[peer], dq_send.at[peer], dq_recv.at[peer], peer).wait_recv()

    def w_copy(h, c, slot):
        return pltpu.make_async_copy(wqf.at[h, pl.ds(c * tile, tile)],
                                     p_ref.at[h, :, pl.ds(slot * width, width)], b_sem.at[slot, h])

    def own_copy(c, slot):
        return pltpu.make_async_copy(wq.at[pl.ds(c * tile, tile)],
                                     p_ref.at[me, :, pl.ds(slot * width, width)], b_sem.at[slot, me])

    def w_load(c, slot):
        own_copy(c, slot).start()
        for d in range(1, n):
            w_copy(lax.rem(me + d, n), c, slot).start()

    w_load(0, 0)
    for c in range(model // tile):
        slot = c % 2
        for h in range(n):
            w_copy(h, c, slot).wait()
        if c + 1 < model // tile:
            w_load(c + 1, 1 - slot)
        s_ref[c] = jnp.zeros_like(s_ref[c])

        def heads(h, _):
            s_ref[c] += _mm_t(dqr[h], p_ref[h, :, slot * width:(slot + 1) * width])
            return _

        lax.fori_loop(0, n, heads, 0)

    rs_wait(dwr, 1, 0, 0)
    acc[1, rb // 2, :, part_cols(0)] += dwr[0, 0]
    rs_start(acc.at[1, rb // 2, :, pl.ds(0, tile // 2)], dwr, 1, 0, 1)
    rs_wait(dwr, 1, 1, 0)
    acc[1, lb // 2, :, part_cols(1)] += dwr[1, 0]
    rs_start(acc.at[1, lb // 2, :, pl.ds(tile // 2, tile // 2)], dwr, 1, 1, 1)

    def q_copy(c):
        return pltpu.make_async_copy(lse.at[pl.ds(2 * c, 2)], dwq.at[pl.ds(2 * c, 2)], l_sem.at[c])

    for c in range(model // tile):
        for g in range(4):
            lse[2 * c + g // 2, pl.ds(g % 2, half, stride=2)] = (
                acc[0, c, (g % 2) * lanes:(g % 2 + 1) * lanes, (g // 2) * half:(g // 2 + 1) * half].T)
        q_copy(c).start()

    rs_wait(kvr, 0, 0, 1)
    rs_wait(kvr, 0, 1, 2)
    stag(base)[...] += kvr[0, 1] + kvr[1, 2]
    rs_wait(kvr, 0, 0, 2)
    rs_wait(kvr, 0, 1, 1)
    stag(base + 1)[...] += kvr[0, 2] + kvr[1, 1]
    swap = _remote(stag(mate), kvx.at[0], b_sem.at[2, 0], b_sem.at[2, 1], mate)
    swap.start()
    kvx[1] = stag(me)[...]
    swap.wait()
    kv_first = kvx[1 - core].T
    kv_second = kvx[core].T

    def split(val):
        hi = val.astype(BF16)
        rest = val - hi.astype(F32)
        mid = rest.astype(BF16)
        lo = (rest - mid.astype(F32)).astype(BF16)
        return hi, mid, lo

    for d in range(1, n):
        peer = lax.rem(me + d, n)
        _remote(dqr.at[peer], dqr.at[peer], dq_send.at[peer], dq_recv.at[peer], peer).wait_send()
    for i, parts in enumerate((split(kv_first), split(kv_second))):
        for g, val in enumerate(parts):
            q[3 * i + g] = val
    for c in range(model // tile):
        at = slice(c * tile, (c + 1) * tile)
        total = s_ref[c]
        for i, w in enumerate((wk_v, wv_v)):
            wt = w[at]
            total += (_mm_t(q[3 * i + 2], wt) + _mm_t(q[3 * i + 1], wt)) + _mm_t(q[3 * i], wt)
        xbuf[0, :, at] = total.astype(BF16)
    out_dx = pltpu.make_async_copy(xbuf.at[0], dx, x_sem.at[0])
    out_dx.start()

    outs = [out_wo, out_dx]
    rs_wait(dwr, 1, 0, 1)
    rs_wait(dwr, 1, 1, 2)
    acc[1, base // 2, :, part_cols(0)] += dwr[0, 1] + dwr[1, 2]
    rs_wait(dwr, 1, 0, 2)
    rs_wait(dwr, 1, 1, 1)
    acc[1, base // 2, :, part_cols(1)] += dwr[0, 2] + dwr[1, 1]
    swap = _remote(part(mate), dwx.at[0], b_sem.at[2, 2], b_sem.at[2, 3], mate)
    swap.start()
    dwx[1] = part(me)[...]
    swap.wait()
    for i, (val, out) in enumerate(((dwx[1 - core].T, dwk), (dwx[core].T, dwv))):
        oacc[i * width:(i + 1) * width] = val
        outs.append(pltpu.make_async_copy(oacc.at[pl.ds(i * width, width)], out, o_sem.at[1 + i]))
        outs[-1].start()
    for c in outs:
        c.wait()
    for c in range(model // tile):
        q_copy(c).wait()

    for c in sends:
        c.wait_send()
    for a in range(2):
        for i in range(3):
            _remote(view(a, me, 0), view(a, me, 0), g_sr.at[a, i], g_recv.at[a, 0], mate).wait_send()
            _remote(view(a, me, 0), view(a, me, 0), g_sl.at[a, i], g_recv.at[a, 0], mate).wait_send()
        for i in range(8):
            _remote(view(a, me, 0), view(a, me, 0), g_sp.at[a, i], g_recv.at[a, 0], mate).wait_send()
    for i in range(3):
        _remote(wview(me, 0), wview(me, 0), w_sr.at[i], w_recv.at[0], mate).wait_send()
        _remote(wview(me, 0), wview(me, 0), w_sl.at[i], w_recv.at[0], mate).wait_send()
    for i in range(8):
        _remote(wview(me, 0), wview(me, 0), w_sp.at[i], w_recv.at[0], mate).wait_send()


def solution(mesh):
    n = mesh.shape["tp"]
    hbm = pl.BlockSpec(memory_space=pl.ANY)
    dma = pltpu.SemaphoreType.DMA

    def local_grads(x_blk, dy_blk, wq_loc, w_k, w_v, wo_loc):
        model, kv_heads, width = w_k.shape
        rows = x_blk.shape[0]
        scale = width ** -0.5
        wq2 = wq_loc.reshape(model, width)
        wk2 = w_k.reshape(model, width)
        wv2 = w_v.reshape(model, width)
        wo2 = wo_loc.reshape(width, model)
        tile = 2 * model // n
        full = jax.ShapeDtypeStruct((n, rows, model), BF16)
        proj = pltpu.VMEM((n, rows, width), BF16)
        dx, dwq, dwo, dwk, dwv, _, _, _ = pl.pallas_call(
            functools.partial(_kernel, n, scale),
            name="attention_grads",
            out_shape=(
                jax.ShapeDtypeStruct((rows, model), BF16),
                jax.ShapeDtypeStruct((n, rows, 128), F32),
                jax.ShapeDtypeStruct((width, model), F32),
                jax.ShapeDtypeStruct((model // n, width), F32),
                jax.ShapeDtypeStruct((model // n, width), F32),
                full, full,
                jax.ShapeDtypeStruct((n, model, width), BF16),
            ),
            in_specs=[hbm] * 6,
            out_specs=(hbm,) * 8,
            scratch_shapes=[
                proj, proj, proj, proj,
                pltpu.VMEM((model, width), BF16),
                pltpu.VMEM((model, width), BF16),
                pltpu.VMEM((model, width), BF16),
                pltpu.VMEM((width, model), BF16),
                pltpu.VMEM((n, rows, rows), F32),
                pltpu.VMEM((n, rows, rows), BF16),
                pltpu.VMEM((2, n, width, rows), F32),
                pltpu.VMEM((n, 3 * width, rows), BF16),
                pltpu.VMEM((n, rows, width), BF16),
                pltpu.VMEM((n, rows, 128), F32),
                pltpu.VMEM((n, rows, width), BF16),
                pltpu.VMEM((2, 3, width, rows), F32),
                pltpu.VMEM((2, width, rows), F32),
                pltpu.VMEM((2, 3, width, tile // 2), F32),
                pltpu.VMEM((2, width, tile // 2), F32),
                pltpu.VMEM((2, rows, model), BF16),
                pltpu.VMEM((rows, 128), F32),
                pltpu.VMEM((rows, 128), F32),
                pltpu.VMEM((rows, width), F32),
                pltpu.VMEM((width, rows), BF16),
                pltpu.VMEM((width, rows), BF16),
                pltpu.VMEM((width, model), F32),
                dma((2, 3)), dma((2, 3)), dma((2, 8)), dma((2, 2 * n)), dma((4,)),
                dma((3,)), dma((3,)), dma((8,)), dma((2 * n,)),
                dma((n,)), dma((n,)), dma((n,)), dma((n,)),
                dma((2, 2, 3)), dma((2, 2, 3)), dma((2,)), dma((3, n)), dma((4,)),
            ],
            compiler_params=pltpu.CompilerParams(
                collective_id=0, has_side_effects=True, vmem_limit_bytes=VMEM_MAX),
        )(x_blk, dy_blk, wq2, wk2, wv2, wo2)
        return (dx, dwq.reshape(model, 1, width), dwo.reshape(1, width, model), dwk, dwv)

    tok_spec = P(("dp", "tp"))
    return jax.shard_map(
        local_grads,
        mesh=mesh,
        in_specs=(tok_spec, tok_spec, P(None, "tp", None), P(), P(), P("tp")),
        out_specs=(tok_spec, P("dp", "tp", None), tok_spec, tok_spec, tok_spec),
        check_vma=False,
    )
```

```python
import functools

import jax
import jax.numpy as jnp
from jax import lax
from jax.experimental import pallas as pl
from jax.experimental.pallas import tpu as pltpu
from jax.sharding import PartitionSpec as P

MESH = pl.DeviceIdType.MESH
F32 = jnp.float32
BF16 = jnp.bfloat16
LOG2E = 1.4426950408889634
VMEM_MAX = 67_043_328


def _mm(a, b):
    return lax.dot_general(a, b, (((1,), (0,)), ((), ())), preferred_element_type=F32)


def _mm_t(a, b):
    return lax.dot_general(a, b, (((1,), (1,)), ((), ())), preferred_element_type=F32)


def _ring(n):
    me = lax.axis_index("tp")
    core = lax.rem(me, 2)
    right = lax.rem(me + 2, n)
    left = lax.rem(me + n - 2, n)
    opp = lax.rem(me + n // 2, n)
    mate = me + 1 - 2 * core
    return me, core, right, left, opp, mate


def _barrier(devices):
    barrier = pltpu.get_barrier_semaphore()
    for d in devices:
        pl.semaphore_signal(barrier, inc=1, device_id=d, device_id_type=MESH)
    pl.semaphore_wait(barrier, len(devices))


def _remote(src, dst, ssem, rsem, dev):
    return pltpu.make_async_remote_copy(
        src_ref=src, dst_ref=dst, send_sem=ssem, recv_sem=rsem,
        device_id={"tp": dev}, device_id_type=MESH)


def _kernel(n, scale, x, dy, wq, wk, wv, wo,
            dx, dwq, dwo, dwk, dwv, xf, dyf, wqf,
            q, k, v, do, wq_v, wk_v, wv_v, wo_v,
            s_ref, p_ref, acc, lhs, o, lse, dqr, kvr, kvx, dwr, dwx, xbuf,
            mrow, lrow, oacc, qt, dot_, dwo_v,
            g_sr, g_sl, g_sp, g_recv, l_sem,
            w_sr, w_sl, w_sp, w_st, w_recv, dq_send, dq_recv, kv_send, kv_recv,
            rs_send, rs_recv, x_sem, b_sem, o_sem):
    me, core, right, left, opp, mate = _ring(n)
    chip = me // 2
    flip = 1 - 2 * core
    blk, width = q.shape[1], q.shape[2]
    half = blk // 2
    model = x.shape[1]
    tile = model // (n // 2)
    lanes = 128
    group = lax.axis_index("dp")
    side = lax.rem(group, 2)
    twin = {"dp": group + 1 - 2 * side, "tp": me}
    _barrier([{"tp": lax.rem(me + d, n)} for d in range(1, n)] + [twin])
    sends = []

    srcs, dsts = (x, dy), (xf, dyf)

    def view(a, b, h):
        return dsts[a].at[b, pl.ds(h * half, half)]

    def send(src, a, b, h, ssem, dev):
        _remote(src, view(a, b, h), ssem, g_recv.at[a, b * 2 + h], dev).start()

    def recv(a, b, h):
        _remote(view(a, b, h), view(a, b, h), g_sp.at[a, 0], g_recv.at[a, b * 2 + h], mate).wait_recv()

    def own(a, h):
        return srcs[a].at[pl.ds(h * half, half)]

    def send_own(a):
        for i, h in enumerate((0, 1)):
            send(own(a, h), a, me, h, g_sr.at[a, i], right)
            send(own(a, 1 - h), a, me, 1 - h, g_sl.at[a, i], left)

    def chunk(i):
        return xbuf.at[i // 2, pl.ds(lax.rem(i, 2) * half, half)]

    def load(src, i):
        return pltpu.make_async_copy(src, chunk(i), l_sem.at[i])

    def project(a, b0, h0, b1, h1):
        def body(i, carry):
            side, par = lax.rem(i, 2), i // 2
            b = b0 + side * (b1 - b0) + par * flip
            h = h0 + side * (h1 - h0)
            load(view(a, b, h), i).wait()
            at = pl.ds(pl.multiple_of(h * half, half), half)
            data = chunk(i)[...]
            if a == 0:
                q[b, at] = _mm(data, wq_v[...]).astype(BF16)
                k[b, at] = _mm(data, wk_v[...]).astype(BF16)
                v[b, at] = _mm(data, wv_v[...]).astype(BF16)
            else:
                do[b, at] = _mm_t(data, wo_v[...]).astype(BF16)
            return carry
        lax.fori_loop(0, 4, body, 0)

    def first(a):
        for h in range(2):
            load(own(a, h), h).start()
        for h in range(2):
            recv(a, mate, h)
            load(view(a, mate, h), 2 + h).start()
        project(a, me, 0, me, 1)

    def event(a, e):
        b0, h0, b1, h1 = ((left, 0, right, 1), (left, 1, right, 0), (opp, 0, opp, 1))[e - 1]
        for i, (b, h) in enumerate(((b0, h0), (b1, h1))):
            recv(a, b, h)
            if e == 1:
                send(view(a, b, h), a, b, h, (g_sr, g_sl)[i].at[a, 2], (right, left)[i])
            send(view(a, b, h), a, b, h, g_sp.at[a, 2 * e + i], mate)
            load(view(a, b, h), i).start()
        if e == 1:
            if a == 0:
                send_own(1)
            else:
                send_wq()
        for i, (b, h) in enumerate(((b0, h0), (b1, h1))):
            recv(a, b + flip, h)
            load(view(a, b + flip, h), 2 + i).start()
        project(a, b0, h0, b1, h1)

    quarter = model // 4

    def wview(b, i):
        return wqf.at[b, pl.ds(i * quarter, quarter)]

    def wcopy(src, b, i, ssem, dev):
        dev = dev if isinstance(dev, dict) else {"tp": dev}
        return pltpu.make_async_remote_copy(
            src_ref=src, dst_ref=wview(b, i), send_sem=ssem, recv_sem=w_recv.at[b, i],
            device_id=dev, device_id_type=MESH)

    def wrecv(b, i):
        wcopy(wview(b, i), b, i, w_sp.at[0], mate).wait_recv()

    def wown(i):
        return wq.at[pl.ds(i * quarter, quarter)]

    mine, other = 2 * side, 2 - 2 * side

    def send_wq():
        for i in range(2):
            wcopy(wown(mine + i), me, mine + i, w_sr.at[i], right).start()
            wcopy(wown(mine + 1 - i), me, mine + 1 - i, w_sl.at[i], left).start()

    def wevent(e):
        pieces = (((left, 0), (right, 1)), ((left, 1), (right, 0)), ((opp, 0), (opp, 1)))[e - 1]
        for g, (b, i) in enumerate(pieces):
            i = mine + i
            wrecv(b, i)
            if e == 1:
                wcopy(wview(b, i), b, i, (w_sr, w_sl)[g].at[2], (right, left)[g]).start()
            wcopy(wview(b, i), b, i, w_sp.at[2 + 2 * e + g], mate).start()
            wcopy(wview(b, i), b, i, w_st.at[2 * e - 2 + g], twin).start()

    def wtwin():
        for g, (b, i) in enumerate(((left, 0), (right, 1), (left, 1), (right, 0), (opp, 0), (opp, 1))):
            i = other + i
            wrecv(b, i)
            wcopy(wview(b, i), b, i, w_sp.at[10 + g], mate).start()

    send_own(0)
    for a in range(2):
        for h in range(2):
            send(own(a, h), a, me, h, g_sp.at[a, h], mate)
    for i in range(4):
        wcopy(wown(i), me, i, w_sp.at[i], mate).start()
    loads = [pltpu.make_async_copy(src, dst, o_sem.at[i])
             for i, (src, dst) in enumerate(((wq, wq_v), (wk, wk_v), (wv, wv_v), (wo, wo_v)))]
    for c in loads:
        c.start()
    acc[...] = jnp.zeros_like(acc)
    dwo_v[...] = jnp.zeros_like(dwo_v)
    for c in loads:
        c.wait()
    first(0)
    for e in (1, 2, 3):
        event(0, e)

    def fold(val, op):
        out = val[:, :lanes]
        for c in range(1, val.shape[1] // lanes):
            out = op(out, val[:, c * lanes:(c + 1) * lanes])
        return out

    def groups(val):
        return [val[:, c * lanes:(c + 1) * lanes] for c in range(val.shape[1] // lanes)]

    def expo(val, top):
        return jnp.exp2((val - top) * (scale * LOG2E))

    keep = (lax.broadcasted_iota(jnp.int32, (blk, blk), 0)
            >= lax.broadcasted_iota(jnp.int32, (blk, blk), 1))

    def forward(nb, carry):
        mrow[...] = jnp.full_like(mrow, jnp.finfo(F32).min)
        lrow[...] = jnp.zeros_like(lrow)

        def stats(j, sc):
            s_ref[j] = sc
            old = mrow[...]
            top = jnp.maximum(old, fold(sc, jnp.maximum))
            total = lrow[...] * expo(old, top)
            for part in groups(sc):
                total += expo(part, top)
            mrow[...] = top
            lrow[...] = total

        def scores(j, carry):
            stats(j, _mm_t(q[nb], k[j]))
            return carry

        lax.fori_loop(0, nb, scores, 0)
        stats(nb, jnp.where(keep, _mm_t(q[nb], k[nb]), -jnp.inf))
        top = jnp.max(mrow[...], axis=1, keepdims=True)
        total = jnp.sum(lrow[...] * expo(mrow[...], top), axis=1, keepdims=True)
        lse[nb] = jnp.broadcast_to(top + jnp.log(total) * (1.0 / scale), mrow.shape)
        oacc[...] = jnp.zeros_like(oacc)

        def values(j, carry):
            shift = lse[nb]
            pb = jnp.concatenate([expo(part, shift).astype(BF16) for part in groups(s_ref[j])], axis=1)
            oacc[...] += _mm(pb, v[j])
            return carry

        lax.fori_loop(0, nb + 1, values, 0)
        o[nb] = oacc[...].astype(BF16)
        return carry

    lax.fori_loop(0, n, forward, 0)

    def q_step(t, carry):
        p = t // 2
        nb = lax.rem(me + 2 * p + 2 * (p // 2) * (1 - 2 * lax.rem(p, 2)), n) + lax.rem(t, 2) * flip

        @pl.when(t == 0)
        def _():
            first(1)
            event(1, 1)

        @pl.when(t == 2)
        def _():
            event(1, 2)

        @pl.when(t == 6)
        def _():
            event(1, 3)

        @pl.when(t == 7)
        def _():
            wevent(1)

        dy_copy = pltpu.make_async_copy(dyf.at[nb], xbuf.at[0], x_sem.at[0])

        @pl.when(t == 0)
        def _():
            pltpu.make_async_copy(dy, xbuf.at[0], x_sem.at[0]).start()

        @pl.when(t > 0)
        def _():
            dy_copy.start()

        qt[...] = q[nb].T
        dot_[...] = do[nb].T
        delta = jnp.sum(do[nb].astype(F32) * o[nb].astype(F32), axis=1, keepdims=True)
        mrow[...] = jnp.broadcast_to(delta, mrow.shape)
        oacc[...] = jnp.zeros_like(oacc)

        def grads(j, mask):
            sc = groups(_mm_t(q[nb], k[j]))
            dp = groups(_mm_t(do[nb], v[j]))
            shift, less = lse[nb], mrow[...]
            pr = [expo(part, shift) for part in sc]
            if mask:
                pr = [jnp.where(kg, part, 0.0) for kg, part in zip(groups(keep), pr)]
            ds = jnp.concatenate([(pp * (dd - less)).astype(BF16) for pp, dd in zip(pr, dp)], axis=1)
            pb = jnp.concatenate([pp.astype(BF16) for pp in pr], axis=1)
            oacc[...] += _mm(ds, k[j])
            acc[0, j] += _mm(qt[...], ds)
            acc[1, j] += _mm(dot_[...], pb)

        def below(j, carry):
            grads(j, False)
            return carry

        lax.fori_loop(0, nb, below, 0)
        grads(nb, True)
        dq = (oacc[...] * scale).astype(BF16)
        q[nb] = dq
        lhs[nb, 0:width] = dq.T

        @pl.when(t > 0)
        def _():
            _remote(q.at[nb], dqr.at[me], dq_send.at[nb], dq_recv.at[me], nb).start()

        @pl.when(t == 0)
        def _():
            dqr[me] = dq

        dy_copy.wait()
        ot = o[nb].T
        for c in range(model // tile):
            at = pl.ds(c * tile, tile)
            dwo_v[:, at] += _mm(ot, xbuf[0, :, at])
        return carry

    lax.fori_loop(0, n, q_step, 0)

    f_mine = jnp.where(core == 0, scale, 1.0).astype(F32)
    f_other = jnp.where(core == 0, 1.0, scale).astype(F32)

    def kv_copy(b):
        return _remote(p_ref.at[b, pl.ds(0, width)], lhs.at[b, pl.ds(2 * width, width)],
                       kv_send.at[b], kv_recv.at[b], mate)

    def convert(i, _):
        b = lax.rem(me - core + n // 2 + i, n)
        p_ref[b, 0:width] = (acc[1 - core, b] * f_other).astype(BF16)
        kv_copy(b).start()
        lhs[b, width:2 * width] = (acc[core, b] * f_mine).astype(BF16)
        return _

    lax.fori_loop(0, n, convert, 0)

    out_wo = pltpu.make_async_copy(dwo_v, dwo, o_sem.at[0])
    out_wo.start()
    half_chips = n // 2

    def stag(b):
        return s_ref.at[half_chips + b // 2, pl.ds(lax.rem(b, 2) * width, width)]

    def pair(b):
        kv_copy(b).wait_recv()
        stag(b)[...] = (lhs[b, width:2 * width].astype(F32)
                        + lhs[b, 2 * width:3 * width].astype(F32))

    base = 2 * chip
    ob_, rb, lb = opp - core, right - core, left - core

    def rs_copy(src, dst, r, side, kind):
        return _remote(src, dst.at[side, kind], rs_send.at[r, side, kind],
                       rs_recv.at[r, side, kind], right if side == 0 else left)

    def rs_start(*args):
        c = rs_copy(*args)
        c.start()
        sends.append(c)

    def rs_wait(dst, r, side, kind):
        rs_copy(dst.at[side, kind], dst, r, side, kind).wait_recv()

    pair(ob_)
    rs_start(stag(ob_), kvr, 0, 0, 0)
    pair(ob_ + 1)
    rs_start(stag(ob_ + 1), kvr, 0, 1, 0)
    pair(rb + 1)
    rs_start(stag(rb + 1), kvr, 0, 0, 2)
    pair(lb)
    rs_start(stag(lb), kvr, 0, 1, 2)
    for b in (rb, lb + 1, base, base + 1):
        pair(b)

    def x_copy(b, slot):
        return pltpu.make_async_copy(xf.at[b], xbuf.at[slot], x_sem.at[slot])

    pltpu.make_async_copy(x, xbuf.at[0], x_sem.at[0]).start()
    wevent(2)

    def x_step(i, carry):
        slot = lax.rem(i, 2)
        b = lax.rem(me + i, n)
        x_copy(b, slot).wait()

        @pl.when(i < n - 1)
        def _():
            x_copy(lax.rem(me + i + 1, n), 1 - slot).start()

        for c in range(model // tile):
            xt = xbuf[slot, :, c * tile:(c + 1) * tile]
            acc[0, c] += _mm(lhs[b, 0:width], xt)
            acc[1, c] += _mm(lhs[b, width:2 * width], xt) + _mm(lhs[b, 2 * width:3 * width], xt)
        return carry

    def clear(c, _):
        acc[0, c] = jnp.zeros_like(acc[0, c])
        acc[1, c] = jnp.zeros_like(acc[1, c])
        return _

    lax.fori_loop(0, half_chips, clear, 0)
    lax.fori_loop(0, n, x_step, 0)
    wevent(3)

    rs_wait(kvr, 0, 0, 0)
    stag(rb)[...] += kvr[0, 0]
    rs_start(stag(rb), kvr, 0, 0, 1)
    rs_wait(kvr, 0, 1, 0)
    stag(lb + 1)[...] += kvr[1, 0]
    rs_start(stag(lb + 1), kvr, 0, 1, 1)

    def part(b):
        return acc.at[1, b // 2, :, pl.ds(lax.rem(b, 2) * (tile // 2), tile // 2)]

    def part_cols(h):
        return slice(h * (tile // 2), (h + 1) * (tile // 2))

    rs_start(acc.at[1, ob_ // 2, :, pl.ds(0, tile // 2)], dwr, 1, 0, 0)
    rs_start(acc.at[1, ob_ // 2, :, pl.ds(tile // 2, tile // 2)], dwr, 1, 1, 0)
    rs_start(acc.at[1, rb // 2, :, pl.ds(tile // 2, tile // 2)], dwr, 1, 0, 2)
    rs_start(acc.at[1, lb // 2, :, pl.ds(0, tile // 2)], dwr, 1, 1, 2)

    for b in range(n):
        kv_copy(b).wait_send()
    wtwin()
    for b in (mate, left + flip, right + flip, opp + flip):
        for i in range(4):
            wrecv(b, i)
    for d in range(1, n):
        peer = lax.rem(me + d, n)
        _remote(dqr.at[peer], dqr.at[peer], dq_send.at[peer], dq_recv.at[peer], peer).wait_recv()

    def w_copy(h, c, slot):
        return pltpu.make_async_copy(wqf.at[h, pl.ds(c * tile, tile)],
                                     p_ref.at[h, :, pl.ds(slot * width, width)], b_sem.at[slot, h])

    def own_copy(c, slot):
        return pltpu.make_async_copy(wq.at[pl.ds(c * tile, tile)],
                                     p_ref.at[me, :, pl.ds(slot * width, width)], b_sem.at[slot, me])

    def w_load(c, slot):
        own_copy(c, slot).start()
        for d in range(1, n):
            w_copy(lax.rem(me + d, n), c, slot).start()

    w_load(0, 0)
    for c in range(model // tile):
        slot = c % 2
        for h in range(n):
            w_copy(h, c, slot).wait()
        if c + 1 < model // tile:
            w_load(c + 1, 1 - slot)
        s_ref[c] = jnp.zeros_like(s_ref[c])

        def heads(h, _):
            s_ref[c] += _mm_t(dqr[h], p_ref[h, :, slot * width:(slot + 1) * width])
            return _

        lax.fori_loop(0, n, heads, 0)

    rs_wait(dwr, 1, 0, 0)
    acc[1, rb // 2, :, part_cols(0)] += dwr[0, 0]
    rs_start(acc.at[1, rb // 2, :, pl.ds(0, tile // 2)], dwr, 1, 0, 1)
    rs_wait(dwr, 1, 1, 0)
    acc[1, lb // 2, :, part_cols(1)] += dwr[1, 0]
    rs_start(acc.at[1, lb // 2, :, pl.ds(tile // 2, tile // 2)], dwr, 1, 1, 1)

    def q_copy(c):
        return pltpu.make_async_copy(lse.at[pl.ds(2 * c, 2)], dwq.at[pl.ds(2 * c, 2)], l_sem.at[c])

    for c in range(model // tile):
        for g in range(4):
            lse[2 * c + g // 2, pl.ds(g % 2, half, stride=2)] = (
                acc[0, c, (g % 2) * lanes:(g % 2 + 1) * lanes, (g // 2) * half:(g // 2 + 1) * half].T)
        q_copy(c).start()

    rs_wait(kvr, 0, 0, 1)
    rs_wait(kvr, 0, 1, 2)
    stag(base)[...] += kvr[0, 1] + kvr[1, 2]
    rs_wait(kvr, 0, 0, 2)
    rs_wait(kvr, 0, 1, 1)
    stag(base + 1)[...] += kvr[0, 2] + kvr[1, 1]
    swap = _remote(stag(mate), kvx.at[0], b_sem.at[2, 0], b_sem.at[2, 1], mate)
    swap.start()
    kvx[1] = stag(me)[...]
    swap.wait()
    kv_first = kvx[1 - core].T
    kv_second = kvx[core].T

    def split(val):
        hi = val.astype(BF16)
        rest = val - hi.astype(F32)
        mid = rest.astype(BF16)
        lo = (rest - mid.astype(F32)).astype(BF16)
        return hi, mid, lo

    for d in range(1, n):
        peer = lax.rem(me + d, n)
        _remote(dqr.at[peer], dqr.at[peer], dq_send.at[peer], dq_recv.at[peer], peer).wait_send()
    for i, parts in enumerate((split(kv_first), split(kv_second))):
        for g, val in enumerate(parts):
            q[3 * i + g] = val
    for c in range(model // tile):
        at = slice(c * tile, (c + 1) * tile)
        total = s_ref[c]
        for i, w in enumerate((wk_v, wv_v)):
            wt = w[at]
            total += (_mm_t(q[3 * i + 2], wt) + _mm_t(q[3 * i + 1], wt)) + _mm_t(q[3 * i], wt)
        xbuf[0, :, at] = total.astype(BF16)
    out_dx = pltpu.make_async_copy(xbuf.at[0], dx, x_sem.at[0])
    out_dx.start()

    outs = [out_wo, out_dx]
    rs_wait(dwr, 1, 0, 1)
    rs_wait(dwr, 1, 1, 2)
    acc[1, base // 2, :, part_cols(0)] += dwr[0, 1] + dwr[1, 2]
    rs_wait(dwr, 1, 0, 2)
    rs_wait(dwr, 1, 1, 1)
    acc[1, base // 2, :, part_cols(1)] += dwr[0, 2] + dwr[1, 1]
    swap = _remote(part(mate), dwx.at[0], b_sem.at[2, 2], b_sem.at[2, 3], mate)
    swap.start()
    dwx[1] = part(me)[...]
    swap.wait()
    for i, (val, out) in enumerate(((dwx[1 - core].T, dwk), (dwx[core].T, dwv))):
        oacc[i * width:(i + 1) * width] = val
        outs.append(pltpu.make_async_copy(oacc.at[pl.ds(i * width, width)], out, o_sem.at[1 + i]))
        outs[-1].start()
    for c in outs:
        c.wait()
    for c in range(model // tile):
        q_copy(c).wait()

    for c in sends:
        c.wait_send()
    for a in range(2):
        for i in range(3):
            _remote(view(a, me, 0), view(a, me, 0), g_sr.at[a, i], g_recv.at[a, 0], mate).wait_send()
            _remote(view(a, me, 0), view(a, me, 0), g_sl.at[a, i], g_recv.at[a, 0], mate).wait_send()
        for i in range(8):
            _remote(view(a, me, 0), view(a, me, 0), g_sp.at[a, i], g_recv.at[a, 0], mate).wait_send()
    for sems, count in ((w_sr, 3), (w_sl, 3), (w_sp, 16), (w_st, 6)):
        for i in range(count):
            wcopy(wview(me, 0), me, 0, sems.at[i], mate).wait_send()


def solution(mesh):
    n = mesh.shape["tp"]
    hbm = pl.BlockSpec(memory_space=pl.ANY)
    dma = pltpu.SemaphoreType.DMA

    def local_grads(x_blk, dy_blk, wq_loc, w_k, w_v, wo_loc):
        model, kv_heads, width = w_k.shape
        rows = x_blk.shape[0]
        scale = width ** -0.5
        wq2 = wq_loc.reshape(model, width)
        wk2 = w_k.reshape(model, width)
        wv2 = w_v.reshape(model, width)
        wo2 = wo_loc.reshape(width, model)
        tile = 2 * model // n
        full = jax.ShapeDtypeStruct((n, rows, model), BF16)
        proj = pltpu.VMEM((n, rows, width), BF16)
        dx, dwq, dwo, dwk, dwv, _, _, _ = pl.pallas_call(
            functools.partial(_kernel, n, scale),
            name="attention_grads",
            out_shape=(
                jax.ShapeDtypeStruct((rows, model), BF16),
                jax.ShapeDtypeStruct((n, rows, 128), F32),
                jax.ShapeDtypeStruct((width, model), F32),
                jax.ShapeDtypeStruct((model // n, width), F32),
                jax.ShapeDtypeStruct((model // n, width), F32),
                full, full,
                jax.ShapeDtypeStruct((n, model, width), BF16),
            ),
            in_specs=[hbm] * 6,
            out_specs=(hbm,) * 8,
            scratch_shapes=[
                proj, proj, proj, proj,
                pltpu.VMEM((model, width), BF16),
                pltpu.VMEM((model, width), BF16),
                pltpu.VMEM((model, width), BF16),
                pltpu.VMEM((width, model), BF16),
                pltpu.VMEM((n, rows, rows), F32),
                pltpu.VMEM((n, rows, rows), BF16),
                pltpu.VMEM((2, n, width, rows), F32),
                pltpu.VMEM((n, 3 * width, rows), BF16),
                pltpu.VMEM((n, rows, width), BF16),
                pltpu.VMEM((n, rows, 128), F32),
                pltpu.VMEM((n, rows, width), BF16),
                pltpu.VMEM((2, 3, width, rows), F32),
                pltpu.VMEM((2, width, rows), F32),
                pltpu.VMEM((2, 3, width, tile // 2), F32),
                pltpu.VMEM((2, width, tile // 2), F32),
                pltpu.VMEM((2, rows, model), BF16),
                pltpu.VMEM((rows, 128), F32),
                pltpu.VMEM((rows, 128), F32),
                pltpu.VMEM((rows, width), F32),
                pltpu.VMEM((width, rows), BF16),
                pltpu.VMEM((width, rows), BF16),
                pltpu.VMEM((width, model), F32),
                dma((2, 3)), dma((2, 3)), dma((2, 8)), dma((2, 2 * n)), dma((4,)),
                dma((3,)), dma((3,)), dma((16,)), dma((6,)), dma((n, 4)),
                dma((n,)), dma((n,)), dma((n,)), dma((n,)),
                dma((2, 2, 3)), dma((2, 2, 3)), dma((2,)), dma((3, n)), dma((4,)),
            ],
            compiler_params=pltpu.CompilerParams(
                collective_id=0, has_side_effects=True, vmem_limit_bytes=VMEM_MAX),
        )(x_blk, dy_blk, wq2, wk2, wv2, wo2)
        return (dx, dwq.reshape(model, 1, width), dwo.reshape(1, width, model), dwk, dwv)

    tok_spec = P(("dp", "tp"))
    return jax.shard_map(
        local_grads,
        mesh=mesh,
        in_specs=(tok_spec, tok_spec, P(None, "tp", None), P(), P(), P("tp")),
        out_specs=(tok_spec, P("dp", "tp", None), tok_spec, tok_spec, tok_spec),
        check_vma=False,
    )
```

```python
import functools

import jax
import jax.numpy as jnp
from jax import lax
from jax.experimental import pallas as pl
from jax.experimental.pallas import tpu as pltpu
from jax.sharding import PartitionSpec as P

MESH = pl.DeviceIdType.MESH
F32 = jnp.float32
BF16 = jnp.bfloat16
LOG2E = 1.4426950408889634
VMEM_MAX = 67_043_328


def _mm(a, b):
    return lax.dot_general(a, b, (((1,), (0,)), ((), ())), preferred_element_type=F32)


def _mm_t(a, b):
    return lax.dot_general(a, b, (((1,), (1,)), ((), ())), preferred_element_type=F32)


def _ring(n):
    me = lax.axis_index("tp")
    core = lax.rem(me, 2)
    right = lax.rem(me + 2, n)
    left = lax.rem(me + n - 2, n)
    opp = lax.rem(me + n // 2, n)
    mate = me + 1 - 2 * core
    return me, core, right, left, opp, mate


def _barrier(devices):
    barrier = pltpu.get_barrier_semaphore()
    for d in devices:
        pl.semaphore_signal(barrier, inc=1, device_id=d, device_id_type=MESH)
    pl.semaphore_wait(barrier, len(devices))


def _remote(src, dst, ssem, rsem, dev):
    return pltpu.make_async_remote_copy(
        src_ref=src, dst_ref=dst, send_sem=ssem, recv_sem=rsem,
        device_id={"tp": dev}, device_id_type=MESH)


def _kernel(n, scale, x, dy, wq, wk, wv, wo,
            dx, dwq, dwo, dwk, dwv, xf, dyf, wqf,
            q, k, v, do, wq_v, wk_v, wv_v, wo_v,
            s_ref, p_ref, acc, lhs, o, lse, dqr, kvr, kvx, dwr, dwx, xbuf,
            mrow, oacc, qt, dot_, dwo_v,
            g_sr, g_sl, g_sp, g_recv, l_sem,
            w_sr, w_sl, w_sp, w_st, w_recv, dq_send, dq_recv, kv_send, kv_recv,
            rs_send, rs_recv, x_sem, b_sem, o_sem):
    me, core, right, left, opp, mate = _ring(n)
    chip = me // 2
    flip = 1 - 2 * core
    blk, width = q.shape[1], q.shape[2]
    half = blk // 2
    model = x.shape[1]
    tile = model // (n // 2)
    lanes = 128
    group = lax.axis_index("dp")
    side = lax.rem(group, 2)
    twin = {"dp": group + 1 - 2 * side, "tp": me}
    _barrier([{"tp": lax.rem(me + d, n)} for d in range(1, n)] + [twin])
    sends = []

    srcs, dsts = (x, dy), (xf, dyf)

    def view(a, b, h):
        return dsts[a].at[b, pl.ds(h * half, half)]

    def send(src, a, b, h, ssem, dev):
        _remote(src, view(a, b, h), ssem, g_recv.at[a, b * 2 + h], dev).start()

    def recv(a, b, h):
        _remote(view(a, b, h), view(a, b, h), g_sp.at[a, 0], g_recv.at[a, b * 2 + h], mate).wait_recv()

    def own(a, h):
        return srcs[a].at[pl.ds(h * half, half)]

    def send_own(a):
        for i, h in enumerate((0, 1)):
            send(own(a, h), a, me, h, g_sr.at[a, i], right)
            send(own(a, 1 - h), a, me, 1 - h, g_sl.at[a, i], left)

    def chunk(i):
        return xbuf.at[i // 2, pl.ds(lax.rem(i, 2) * half, half)]

    def load(src, i):
        return pltpu.make_async_copy(src, chunk(i), l_sem.at[i])

    def project(a, b0, h0, b1, h1):
        def body(i, carry):
            side, par = lax.rem(i, 2), i // 2
            b = b0 + side * (b1 - b0) + par * flip
            h = h0 + side * (h1 - h0)
            load(view(a, b, h), i).wait()
            at = pl.ds(pl.multiple_of(h * half, half), half)
            data = chunk(i)[...]
            if a == 0:
                q[b, at] = _mm(data, wq_v[...]).astype(BF16)
                k[b, at] = _mm(data, wk_v[...]).astype(BF16)
                v[b, at] = _mm(data, wv_v[...]).astype(BF16)
            else:
                do[b, at] = _mm_t(data, wo_v[...]).astype(BF16)
            return carry
        lax.fori_loop(0, 4, body, 0)

    def first(a):
        for h in range(2):
            load(own(a, h), h).start()
        for h in range(2):
            recv(a, mate, h)
            load(view(a, mate, h), 2 + h).start()
        project(a, me, 0, me, 1)

    def event(a, e):
        b0, h0, b1, h1 = ((left, 0, right, 1), (left, 1, right, 0), (opp, 0, opp, 1))[e - 1]
        for i, (b, h) in enumerate(((b0, h0), (b1, h1))):
            recv(a, b, h)
            if e == 1:
                send(view(a, b, h), a, b, h, (g_sr, g_sl)[i].at[a, 2], (right, left)[i])
            send(view(a, b, h), a, b, h, g_sp.at[a, 2 * e + i], mate)
            load(view(a, b, h), i).start()
        if e == 1:
            if a == 0:
                send_own(1)
            else:
                send_wq()
        for i, (b, h) in enumerate(((b0, h0), (b1, h1))):
            recv(a, b + flip, h)
            load(view(a, b + flip, h), 2 + i).start()
        project(a, b0, h0, b1, h1)

    quarter = model // 4

    def wview(b, i):
        return wqf.at[b, pl.ds(i * quarter, quarter)]

    def wcopy(src, b, i, ssem, dev):
        dev = dev if isinstance(dev, dict) else {"tp": dev}
        return pltpu.make_async_remote_copy(
            src_ref=src, dst_ref=wview(b, i), send_sem=ssem, recv_sem=w_recv.at[b, i],
            device_id=dev, device_id_type=MESH)

    def wrecv(b, i):
        wcopy(wview(b, i), b, i, w_sp.at[0], mate).wait_recv()

    def wown(i):
        return wq.at[pl.ds(i * quarter, quarter)]

    mine, other = 2 * side, 2 - 2 * side

    def send_wq():
        for i in range(2):
            wcopy(wown(mine + i), me, mine + i, w_sr.at[i], right).start()
            wcopy(wown(mine + 1 - i), me, mine + 1 - i, w_sl.at[i], left).start()

    def wevent(e):
        pieces = (((left, 0), (right, 1)), ((left, 1), (right, 0)), ((opp, 0), (opp, 1)))[e - 1]
        for g, (b, i) in enumerate(pieces):
            i = mine + i
            wrecv(b, i)
            if e == 1:
                wcopy(wview(b, i), b, i, (w_sr, w_sl)[g].at[2], (right, left)[g]).start()
            wcopy(wview(b, i), b, i, w_sp.at[2 + 2 * e + g], mate).start()
            wcopy(wview(b, i), b, i, w_st.at[2 * e - 2 + g], twin).start()

    def wtwin():
        for g, (b, i) in enumerate(((left, 0), (right, 1), (left, 1), (right, 0), (opp, 0), (opp, 1))):
            i = other + i
            wrecv(b, i)
            wcopy(wview(b, i), b, i, w_sp.at[10 + g], mate).start()

    send_own(0)
    for a in range(2):
        for h in range(2):
            send(own(a, h), a, me, h, g_sp.at[a, h], mate)
    for i in range(4):
        wcopy(wown(i), me, i, w_sp.at[i], mate).start()
    loads = [pltpu.make_async_copy(src, dst, o_sem.at[i])
             for i, (src, dst) in enumerate(((wq, wq_v), (wk, wk_v), (wv, wv_v), (wo, wo_v)))]
    for c in loads:
        c.start()
    acc[...] = jnp.zeros_like(acc)
    dwo_v[...] = jnp.zeros_like(dwo_v)
    for c in loads:
        c.wait()

    def fold(val, op):
        out = val[:, :lanes]
        for c in range(1, val.shape[1] // lanes):
            out = op(out, val[:, c * lanes:(c + 1) * lanes])
        return out

    def groups(val):
        return [val[:, c * lanes:(c + 1) * lanes] for c in range(val.shape[1] // lanes)]

    def expo(val, top):
        return jnp.exp2((val - top) * (scale * LOG2E))

    keep = (lax.broadcasted_iota(jnp.int32, (blk, blk), 0)
            >= lax.broadcasted_iota(jnp.int32, (blk, blk), 1))

    def order(t):
        p = t // 2
        return lax.rem(me + 2 * p + 2 * (p // 2) * (1 - 2 * lax.rem(p, 2)), n) + lax.rem(t, 2) * flip

    def stats(nb, j, mask):
        sc = _mm_t(q[nb], k[j])
        if mask:
            sc = jnp.where(keep, sc, -jnp.inf)
        old = lse[nb]
        top = jnp.maximum(old, fold(sc, jnp.maximum))
        total = s_ref[nb, :, 0:lanes] * expo(old, top)
        for part in groups(sc):
            total += expo(part, top)
        lse[nb] = top
        s_ref[nb, :, 0:lanes] = total

    def land(t, carry):
        @pl.when(t == 0)
        def _():
            first(0)

        @pl.when(t == 2)
        def _():
            event(0, 1)
            event(0, 2)

        @pl.when(t == 6)
        def _():
            event(0, 3)

        nb = order(t)

        def against(i, carry):
            b = order(i)
            stats(jnp.maximum(nb, b), jnp.minimum(nb, b), False)
            return carry

        lax.fori_loop(0, t, against, 0)
        stats(nb, nb, True)
        return carry

    lse[...] = jnp.full_like(lse, jnp.finfo(F32).min)
    s_ref[:, :, 0:lanes] = jnp.zeros((n, blk, lanes), F32)
    lax.fori_loop(0, n, land, 0)

    def forward(nb, carry):
        peak = lse[nb]
        top = jnp.max(peak, axis=1, keepdims=True)
        total = jnp.sum(s_ref[nb, :, 0:lanes] * expo(peak, top), axis=1, keepdims=True)
        lse[nb] = jnp.broadcast_to(top + jnp.log(total) * (1.0 / scale), (blk, lanes))
        oacc[...] = jnp.zeros_like(oacc)

        def values(j, mask):
            shift = lse[nb]
            pr = [expo(part, shift) for part in groups(_mm_t(q[nb], k[j]))]
            if mask:
                pr = [jnp.where(kg, part, 0.0) for kg, part in zip(groups(keep), pr)]
            oacc[...] += _mm(jnp.concatenate([part.astype(BF16) for part in pr], axis=1), v[j])

        def below(j, carry):
            values(j, False)
            return carry

        lax.fori_loop(0, nb, below, 0)
        values(nb, True)
        o[nb] = oacc[...].astype(BF16)
        return carry

    lax.fori_loop(0, n, forward, 0)

    def q_step(t, carry):
        nb = order(t)

        @pl.when(t == 0)
        def _():
            first(1)
            event(1, 1)

        @pl.when(t == 2)
        def _():
            event(1, 2)

        @pl.when(t == 6)
        def _():
            event(1, 3)

        @pl.when(t == 7)
        def _():
            wevent(1)

        qt[...] = q[nb].T
        dot_[...] = do[nb].T
        delta = jnp.sum(do[nb].astype(F32) * o[nb].astype(F32), axis=1, keepdims=True)
        mrow[...] = jnp.broadcast_to(delta, mrow.shape)
        oacc[...] = jnp.zeros_like(oacc)

        def grads(j, mask):
            sc = groups(_mm_t(q[nb], k[j]))
            dp = groups(_mm_t(do[nb], v[j]))
            shift, less = lse[nb], mrow[...]
            pr = [expo(part, shift) for part in sc]
            if mask:
                pr = [jnp.where(kg, part, 0.0) for kg, part in zip(groups(keep), pr)]
            ds = jnp.concatenate([(pp * (dd - less)).astype(BF16) for pp, dd in zip(pr, dp)], axis=1)
            pb = jnp.concatenate([pp.astype(BF16) for pp in pr], axis=1)
            oacc[...] += _mm(ds, k[j])
            acc[0, j] += _mm(qt[...], ds)
            acc[1, j] += _mm(dot_[...], pb)

        def below(j, carry):
            grads(j, False)
            return carry

        lax.fori_loop(0, nb, below, 0)
        grads(nb, True)
        dq = (oacc[...] * scale).astype(BF16)
        q[nb] = dq
        lhs[nb, 0:width] = dq.T

        @pl.when(t > 0)
        def _():
            _remote(q.at[nb], dqr.at[me], dq_send.at[nb], dq_recv.at[me], nb).start()

        @pl.when(t == 0)
        def _():
            dqr[me] = dq

        return carry

    lax.fori_loop(0, n, q_step, 0)

    f_mine = jnp.where(core == 0, scale, 1.0).astype(F32)
    f_other = jnp.where(core == 0, 1.0, scale).astype(F32)

    def kv_copy(b):
        return _remote(p_ref.at[b, pl.ds(0, width)], lhs.at[b, pl.ds(2 * width, width)],
                       kv_send.at[b], kv_recv.at[b], mate)

    def convert(i, _):
        b = lax.rem(me - core + n // 2 + i, n)
        p_ref[b, 0:width] = (acc[1 - core, b] * f_other).astype(BF16)
        kv_copy(b).start()
        lhs[b, width:2 * width] = (acc[core, b] * f_mine).astype(BF16)
        return _

    lax.fori_loop(0, n, convert, 0)

    half_chips = n // 2

    def stag(b):
        return s_ref.at[half_chips + b // 2, pl.ds(lax.rem(b, 2) * width, width)]

    def pair(b):
        kv_copy(b).wait_recv()
        stag(b)[...] = (lhs[b, width:2 * width].astype(F32)
                        + lhs[b, 2 * width:3 * width].astype(F32))

    base = 2 * chip
    ob_, rb, lb = opp - core, right - core, left - core

    def rs_copy(src, dst, r, side, kind):
        return _remote(src, dst.at[side, kind], rs_send.at[r, side, kind],
                       rs_recv.at[r, side, kind], right if side == 0 else left)

    def rs_start(*args):
        c = rs_copy(*args)
        c.start()
        sends.append(c)

    def rs_wait(dst, r, side, kind):
        rs_copy(dst.at[side, kind], dst, r, side, kind).wait_recv()

    pair(ob_)
    rs_start(stag(ob_), kvr, 0, 0, 0)
    pair(ob_ + 1)
    rs_start(stag(ob_ + 1), kvr, 0, 1, 0)
    pair(rb + 1)
    rs_start(stag(rb + 1), kvr, 0, 0, 2)
    pair(lb)
    rs_start(stag(lb), kvr, 0, 1, 2)
    for b in (rb, lb + 1, base, base + 1):
        pair(b)

    def x_copy(b, slot):
        return pltpu.make_async_copy(xf.at[b], xbuf.at[slot], x_sem.at[slot])

    pltpu.make_async_copy(x, xbuf.at[0], x_sem.at[0]).start()
    wevent(2)

    def x_step(i, carry):
        slot = lax.rem(i, 2)
        b = lax.rem(me + i, n)
        x_copy(b, slot).wait()

        @pl.when(i < n - 1)
        def _():
            x_copy(lax.rem(me + i + 1, n), 1 - slot).start()

        for c in range(model // tile):
            xt = xbuf[slot, :, c * tile:(c + 1) * tile]
            acc[0, c] += _mm(lhs[b, 0:width], xt)
            acc[1, c] += _mm(lhs[b, width:2 * width], xt) + _mm(lhs[b, 2 * width:3 * width], xt)
        return carry

    def clear(c, _):
        acc[0, c] = jnp.zeros_like(acc[0, c])
        acc[1, c] = jnp.zeros_like(acc[1, c])
        return _

    lax.fori_loop(0, half_chips, clear, 0)
    lax.fori_loop(0, n, x_step, 0)
    wevent(3)

    rs_wait(kvr, 0, 0, 0)
    stag(rb)[...] += kvr[0, 0]
    rs_start(stag(rb), kvr, 0, 0, 1)
    rs_wait(kvr, 0, 1, 0)
    stag(lb + 1)[...] += kvr[1, 0]
    rs_start(stag(lb + 1), kvr, 0, 1, 1)

    def part(b):
        return acc.at[1, b // 2, :, pl.ds(lax.rem(b, 2) * (tile // 2), tile // 2)]

    def part_cols(h):
        return slice(h * (tile // 2), (h + 1) * (tile // 2))

    rs_start(acc.at[1, ob_ // 2, :, pl.ds(0, tile // 2)], dwr, 1, 0, 0)
    rs_start(acc.at[1, ob_ // 2, :, pl.ds(tile // 2, tile // 2)], dwr, 1, 1, 0)
    rs_start(acc.at[1, rb // 2, :, pl.ds(tile // 2, tile // 2)], dwr, 1, 0, 2)
    rs_start(acc.at[1, lb // 2, :, pl.ds(0, tile // 2)], dwr, 1, 1, 2)

    def y_copy(b, slot):
        return pltpu.make_async_copy(dyf.at[b], xbuf.at[slot], x_sem.at[slot])

    pltpu.make_async_copy(dy, xbuf.at[0], x_sem.at[0]).start()

    def y_step(i, carry):
        slot = lax.rem(i, 2)
        b = lax.rem(me + i, n)
        ot = o[b].T
        y_copy(b, slot).wait()

        @pl.when(i < n - 1)
        def _():
            y_copy(lax.rem(me + i + 1, n), 1 - slot).start()

        for c in range(model // tile):
            at = pl.ds(c * tile, tile)
            dwo_v[:, at] += _mm(ot, xbuf[slot, :, at])
        return carry

    lax.fori_loop(0, n, y_step, 0)
    out_wo = pltpu.make_async_copy(dwo_v, dwo, o_sem.at[0])
    out_wo.start()

    for b in range(n):
        kv_copy(b).wait_send()
    wtwin()
    for b in (mate, left + flip, right + flip, opp + flip):
        for i in range(4):
            wrecv(b, i)
    for d in range(1, n):
        peer = lax.rem(me + d, n)
        _remote(dqr.at[peer], dqr.at[peer], dq_send.at[peer], dq_recv.at[peer], peer).wait_recv()

    def w_copy(h, c, slot):
        return pltpu.make_async_copy(wqf.at[h, pl.ds(c * tile, tile)],
                                     p_ref.at[h, :, pl.ds(slot * width, width)], b_sem.at[slot, h])

    def own_copy(c, slot):
        return pltpu.make_async_copy(wq.at[pl.ds(c * tile, tile)],
                                     p_ref.at[me, :, pl.ds(slot * width, width)], b_sem.at[slot, me])

    def w_load(c, slot):
        own_copy(c, slot).start()
        for d in range(1, n):
            w_copy(lax.rem(me + d, n), c, slot).start()

    w_load(0, 0)
    for c in range(model // tile):
        slot = c % 2
        for h in range(n):
            w_copy(h, c, slot).wait()
        if c + 1 < model // tile:
            w_load(c + 1, 1 - slot)
        s_ref[c] = jnp.zeros_like(s_ref[c])

        def heads(h, _):
            s_ref[c] += _mm_t(dqr[h], p_ref[h, :, slot * width:(slot + 1) * width])
            return _

        lax.fori_loop(0, n, heads, 0)

    rs_wait(dwr, 1, 0, 0)
    acc[1, rb // 2, :, part_cols(0)] += dwr[0, 0]
    rs_start(acc.at[1, rb // 2, :, pl.ds(0, tile // 2)], dwr, 1, 0, 1)
    rs_wait(dwr, 1, 1, 0)
    acc[1, lb // 2, :, part_cols(1)] += dwr[1, 0]
    rs_start(acc.at[1, lb // 2, :, pl.ds(tile // 2, tile // 2)], dwr, 1, 1, 1)

    def q_copy(c):
        return pltpu.make_async_copy(lse.at[pl.ds(2 * c, 2)], dwq.at[pl.ds(2 * c, 2)], l_sem.at[c])

    for c in range(model // tile):
        for g in range(4):
            lse[2 * c + g // 2, pl.ds(g % 2, half, stride=2)] = (
                acc[0, c, (g % 2) * lanes:(g % 2 + 1) * lanes, (g // 2) * half:(g // 2 + 1) * half].T)
        q_copy(c).start()

    rs_wait(kvr, 0, 0, 1)
    rs_wait(kvr, 0, 1, 2)
    stag(base)[...] += kvr[0, 1] + kvr[1, 2]
    rs_wait(kvr, 0, 0, 2)
    rs_wait(kvr, 0, 1, 1)
    stag(base + 1)[...] += kvr[0, 2] + kvr[1, 1]
    swap = _remote(stag(mate), kvx.at[0], b_sem.at[2, 0], b_sem.at[2, 1], mate)
    swap.start()
    kvx[1] = stag(me)[...]
    swap.wait()
    kv_first = kvx[1 - core].T
    kv_second = kvx[core].T

    def split(val):
        hi = val.astype(BF16)
        rest = val - hi.astype(F32)
        mid = rest.astype(BF16)
        lo = (rest - mid.astype(F32)).astype(BF16)
        return hi, mid, lo

    for d in range(1, n):
        peer = lax.rem(me + d, n)
        _remote(dqr.at[peer], dqr.at[peer], dq_send.at[peer], dq_recv.at[peer], peer).wait_send()
    for i, parts in enumerate((split(kv_first), split(kv_second))):
        for g, val in enumerate(parts):
            q[3 * i + g] = val
    for c in range(model // tile):
        at = slice(c * tile, (c + 1) * tile)
        total = s_ref[c]
        for i, w in enumerate((wk_v, wv_v)):
            wt = w[at]
            total += (_mm_t(q[3 * i + 2], wt) + _mm_t(q[3 * i + 1], wt)) + _mm_t(q[3 * i], wt)
        xbuf[0, :, at] = total.astype(BF16)
    out_dx = pltpu.make_async_copy(xbuf.at[0], dx, x_sem.at[0])
    out_dx.start()

    outs = [out_wo, out_dx]
    rs_wait(dwr, 1, 0, 1)
    rs_wait(dwr, 1, 1, 2)
    acc[1, base // 2, :, part_cols(0)] += dwr[0, 1] + dwr[1, 2]
    rs_wait(dwr, 1, 0, 2)
    rs_wait(dwr, 1, 1, 1)
    acc[1, base // 2, :, part_cols(1)] += dwr[0, 2] + dwr[1, 1]
    swap = _remote(part(mate), dwx.at[0], b_sem.at[2, 2], b_sem.at[2, 3], mate)
    swap.start()
    dwx[1] = part(me)[...]
    swap.wait()
    for i, (val, out) in enumerate(((dwx[1 - core].T, dwk), (dwx[core].T, dwv))):
        oacc[i * width:(i + 1) * width] = val
        outs.append(pltpu.make_async_copy(oacc.at[pl.ds(i * width, width)], out, o_sem.at[1 + i]))
        outs[-1].start()
    for c in outs:
        c.wait()
    for c in range(model // tile):
        q_copy(c).wait()

    for c in sends:
        c.wait_send()
    for a in range(2):
        for i in range(3):
            _remote(view(a, me, 0), view(a, me, 0), g_sr.at[a, i], g_recv.at[a, 0], mate).wait_send()
            _remote(view(a, me, 0), view(a, me, 0), g_sl.at[a, i], g_recv.at[a, 0], mate).wait_send()
        for i in range(8):
            _remote(view(a, me, 0), view(a, me, 0), g_sp.at[a, i], g_recv.at[a, 0], mate).wait_send()
    for sems, count in ((w_sr, 3), (w_sl, 3), (w_sp, 16), (w_st, 6)):
        for i in range(count):
            wcopy(wview(me, 0), me, 0, sems.at[i], mate).wait_send()


def solution(mesh):
    n = mesh.shape["tp"]
    hbm = pl.BlockSpec(memory_space=pl.ANY)
    dma = pltpu.SemaphoreType.DMA

    def local_grads(x_blk, dy_blk, wq_loc, w_k, w_v, wo_loc):
        model, kv_heads, width = w_k.shape
        rows = x_blk.shape[0]
        scale = width ** -0.5
        wq2 = wq_loc.reshape(model, width)
        wk2 = w_k.reshape(model, width)
        wv2 = w_v.reshape(model, width)
        wo2 = wo_loc.reshape(width, model)
        tile = 2 * model // n
        full = jax.ShapeDtypeStruct((n, rows, model), BF16)
        proj = pltpu.VMEM((n, rows, width), BF16)
        dx, dwq, dwo, dwk, dwv, _, _, _ = pl.pallas_call(
            functools.partial(_kernel, n, scale),
            name="attention_grads",
            out_shape=(
                jax.ShapeDtypeStruct((rows, model), BF16),
                jax.ShapeDtypeStruct((n, rows, 128), F32),
                jax.ShapeDtypeStruct((width, model), F32),
                jax.ShapeDtypeStruct((model // n, width), F32),
                jax.ShapeDtypeStruct((model // n, width), F32),
                full, full,
                jax.ShapeDtypeStruct((n, model, width), BF16),
            ),
            in_specs=[hbm] * 6,
            out_specs=(hbm,) * 8,
            scratch_shapes=[
                proj, proj, proj, proj,
                pltpu.VMEM((model, width), BF16),
                pltpu.VMEM((model, width), BF16),
                pltpu.VMEM((model, width), BF16),
                pltpu.VMEM((width, model), BF16),
                pltpu.VMEM((n, rows, rows), F32),
                pltpu.VMEM((n, rows, rows), BF16),
                pltpu.VMEM((2, n, width, rows), F32),
                pltpu.VMEM((n, 3 * width, rows), BF16),
                pltpu.VMEM((n, rows, width), BF16),
                pltpu.VMEM((n, rows, 128), F32),
                pltpu.VMEM((n, rows, width), BF16),
                pltpu.VMEM((2, 3, width, rows), F32),
                pltpu.VMEM((2, width, rows), F32),
                pltpu.VMEM((2, 3, width, tile // 2), F32),
                pltpu.VMEM((2, width, tile // 2), F32),
                pltpu.VMEM((2, rows, model), BF16),
                pltpu.VMEM((rows, 128), F32),
                pltpu.VMEM((rows, width), F32),
                pltpu.VMEM((width, rows), BF16),
                pltpu.VMEM((width, rows), BF16),
                pltpu.VMEM((width, model), F32),
                dma((2, 3)), dma((2, 3)), dma((2, 8)), dma((2, 2 * n)), dma((4,)),
                dma((3,)), dma((3,)), dma((16,)), dma((6,)), dma((n, 4)),
                dma((n,)), dma((n,)), dma((n,)), dma((n,)),
                dma((2, 2, 3)), dma((2, 2, 3)), dma((2,)), dma((3, n)), dma((4,)),
            ],
            compiler_params=pltpu.CompilerParams(
                collective_id=0, has_side_effects=True, vmem_limit_bytes=VMEM_MAX),
        )(x_blk, dy_blk, wq2, wk2, wv2, wo2)
        return (dx, dwq.reshape(model, 1, width), dwo.reshape(1, width, model), dwk, dwv)

    tok_spec = P(("dp", "tp"))
    return jax.shard_map(
        local_grads,
        mesh=mesh,
        in_specs=(tok_spec, tok_spec, P(None, "tp", None), P(), P(), P("tp")),
        out_specs=(tok_spec, P("dp", "tp", None), tok_spec, tok_spec, tok_spec),
        check_vma=False,
    )
```

```python
import functools

import jax
import jax.numpy as jnp
from jax import lax
from jax.experimental import pallas as pl
from jax.experimental.pallas import tpu as pltpu
from jax.sharding import PartitionSpec as P

MESH = pl.DeviceIdType.MESH
F32 = jnp.float32
BF16 = jnp.bfloat16
LOG2E = 1.4426950408889634
VMEM_MAX = 67_043_328


def _mm(a, b):
    return lax.dot_general(a, b, (((1,), (0,)), ((), ())), preferred_element_type=F32)


def _mm_t(a, b):
    return lax.dot_general(a, b, (((1,), (1,)), ((), ())), preferred_element_type=F32)


def _ring(n):
    me = lax.axis_index("tp")
    core = lax.rem(me, 2)
    right = lax.rem(me + 2, n)
    left = lax.rem(me + n - 2, n)
    opp = lax.rem(me + n // 2, n)
    mate = me + 1 - 2 * core
    return me, core, right, left, opp, mate


def _barrier(devices):
    barrier = pltpu.get_barrier_semaphore()
    for d in devices:
        pl.semaphore_signal(barrier, inc=1, device_id=d, device_id_type=MESH)
    pl.semaphore_wait(barrier, len(devices))


def _remote(src, dst, ssem, rsem, dev):
    return pltpu.make_async_remote_copy(
        src_ref=src, dst_ref=dst, send_sem=ssem, recv_sem=rsem,
        device_id={"tp": dev}, device_id_type=MESH)


def _kernel(n, scale, x, dy, wq, wk, wv, wo,
            dx, dwq, dwo, dwk, dwv, xf, dyf, wqf,
            q, k, v, do, wq_v, wk_v, wv_v, wo_v,
            s_ref, p_ref, acc, lhs, o, lse, dqr, kvr, kvx, dwr, dwx, xbuf,
            mrow, oacc, qt, dot_, dwo_v,
            g_sr, g_sl, g_sp, g_recv, l_sem,
            w_sr, w_sl, w_sp, w_st, w_recv, dq_send, dq_recv, kv_send, kv_recv,
            rs_send, rs_recv, x_sem, b_sem, o_sem, y_sem):
    me, core, right, left, opp, mate = _ring(n)
    chip = me // 2
    flip = 1 - 2 * core
    blk, width = q.shape[1], q.shape[2]
    half = blk // 2
    model = x.shape[1]
    tile = model // (n // 2)
    lanes = 128
    group = lax.axis_index("dp")
    side = lax.rem(group, 2)
    twin = {"dp": group + 1 - 2 * side, "tp": me}
    _barrier([{"tp": lax.rem(me + d, n)} for d in range(1, n)] + [twin])
    sends = []

    srcs, dsts = (x, dy), (xf, dyf)

    def view(a, b, h):
        return dsts[a].at[b, pl.ds(h * half, half)]

    def send(src, a, b, h, ssem, dev):
        _remote(src, view(a, b, h), ssem, g_recv.at[a, b * 2 + h], dev).start()

    def recv(a, b, h):
        _remote(view(a, b, h), view(a, b, h), g_sp.at[a, 0], g_recv.at[a, b * 2 + h], mate).wait_recv()

    def own(a, h):
        return srcs[a].at[pl.ds(h * half, half)]

    def send_own(a):
        for i, h in enumerate((0, 1)):
            send(own(a, h), a, me, h, g_sr.at[a, i], right)
            send(own(a, 1 - h), a, me, 1 - h, g_sl.at[a, i], left)

    def chunk(i):
        return xbuf.at[i // 2, pl.ds(lax.rem(i, 2) * half, half)]

    def load(src, i):
        return pltpu.make_async_copy(src, chunk(i), l_sem.at[i])

    def project(a, b0, h0, b1, h1):
        def body(i, carry):
            side, par = lax.rem(i, 2), i // 2
            b = b0 + side * (b1 - b0) + par * flip
            h = h0 + side * (h1 - h0)
            load(view(a, b, h), i).wait()
            at = pl.ds(pl.multiple_of(h * half, half), half)
            data = chunk(i)[...]
            if a == 0:
                q[b, at] = _mm(data, wq_v[...]).astype(BF16)
                k[b, at] = _mm(data, wk_v[...]).astype(BF16)
                v[b, at] = _mm(data, wv_v[...]).astype(BF16)
            else:
                do[b, at] = _mm_t(data, wo_v[...]).astype(BF16)
            return carry
        lax.fori_loop(0, 4, body, 0)

    def first(a):
        for h in range(2):
            load(own(a, h), h).start()
        for h in range(2):
            recv(a, mate, h)
            load(view(a, mate, h), 2 + h).start()
        project(a, me, 0, me, 1)

    def event(a, e):
        b0, h0, b1, h1 = ((left, 0, right, 1), (left, 1, right, 0), (opp, 0, opp, 1))[e - 1]
        for i, (b, h) in enumerate(((b0, h0), (b1, h1))):
            recv(a, b, h)
            if e == 1:
                send(view(a, b, h), a, b, h, (g_sr, g_sl)[i].at[a, 2], (right, left)[i])
            send(view(a, b, h), a, b, h, g_sp.at[a, 2 * e + i], mate)
            load(view(a, b, h), i).start()
        if e == 1:
            if a == 0:
                send_own(1)
            else:
                send_wq()
        for i, (b, h) in enumerate(((b0, h0), (b1, h1))):
            recv(a, b + flip, h)
            load(view(a, b + flip, h), 2 + i).start()
        project(a, b0, h0, b1, h1)

    quarter = model // 4

    def wview(b, i):
        return wqf.at[b, pl.ds(i * quarter, quarter)]

    def wcopy(src, b, i, ssem, dev):
        dev = dev if isinstance(dev, dict) else {"tp": dev}
        return pltpu.make_async_remote_copy(
            src_ref=src, dst_ref=wview(b, i), send_sem=ssem, recv_sem=w_recv.at[b, i],
            device_id=dev, device_id_type=MESH)

    def wrecv(b, i):
        wcopy(wview(b, i), b, i, w_sp.at[0], mate).wait_recv()

    def wown(i):
        return wq.at[pl.ds(i * quarter, quarter)]

    mine, other = 2 * side, 2 - 2 * side

    def send_wq():
        for i in range(2):
            wcopy(wown(mine + i), me, mine + i, w_sr.at[i], right).start()
            wcopy(wown(mine + 1 - i), me, mine + 1 - i, w_sl.at[i], left).start()

    def wevent(e):
        pieces = (((left, 0), (right, 1)), ((left, 1), (right, 0)), ((opp, 0), (opp, 1)))[e - 1]
        for g, (b, i) in enumerate(pieces):
            i = mine + i
            wrecv(b, i)
            if e == 1:
                wcopy(wview(b, i), b, i, (w_sr, w_sl)[g].at[2], (right, left)[g]).start()
            wcopy(wview(b, i), b, i, w_sp.at[2 + 2 * e + g], mate).start()
            wcopy(wview(b, i), b, i, w_st.at[2 * e - 2 + g], twin).start()

    def wtwin():
        for g, (b, i) in enumerate(((left, 0), (right, 1), (left, 1), (right, 0), (opp, 0), (opp, 1))):
            i = other + i
            wrecv(b, i)
            wcopy(wview(b, i), b, i, w_sp.at[10 + g], mate).start()

    send_own(0)
    for a in range(2):
        for h in range(2):
            send(own(a, h), a, me, h, g_sp.at[a, h], mate)
    for i in range(4):
        wcopy(wown(i), me, i, w_sp.at[i], mate).start()
    loads = [pltpu.make_async_copy(src, dst, o_sem.at[i])
             for i, (src, dst) in enumerate(((wq, wq_v), (wk, wk_v), (wv, wv_v), (wo, wo_v)))]
    for c in loads:
        c.start()
    acc[...] = jnp.zeros_like(acc)
    dwo_v[...] = jnp.zeros_like(dwo_v)
    for c in loads:
        c.wait()

    def fold(val, op):
        out = val[:, :lanes]
        for c in range(1, val.shape[1] // lanes):
            out = op(out, val[:, c * lanes:(c + 1) * lanes])
        return out

    def groups(val):
        return [val[:, c * lanes:(c + 1) * lanes] for c in range(val.shape[1] // lanes)]

    def expo(val, top):
        return jnp.exp2((val - top) * (scale * LOG2E))

    keep = (lax.broadcasted_iota(jnp.int32, (blk, blk), 0)
            >= lax.broadcasted_iota(jnp.int32, (blk, blk), 1))

    def order(t):
        p = t // 2
        return lax.rem(me + 2 * p + 2 * (p // 2) * (1 - 2 * lax.rem(p, 2)), n) + lax.rem(t, 2) * flip

    def sums(nb):
        return jnp.concatenate([dwo_v[nb, :, 0:lanes], dwo_v[nb, :, lanes:2 * lanes]], axis=0)

    def stats(nb, j, mask):
        sc = _mm_t(q[nb], k[j])
        if mask:
            sc = jnp.where(keep, sc, -jnp.inf)
        old = lse[nb]
        top = jnp.maximum(old, fold(sc, jnp.maximum))
        total = sums(nb) * expo(old, top)
        for part in groups(sc):
            total += expo(part, top)
        lse[nb] = top
        dwo_v[nb, :, 0:lanes] = total[:half]
        dwo_v[nb, :, lanes:2 * lanes] = total[half:]

    def land(t, carry):
        @pl.when(t == 0)
        def _():
            first(0)

        @pl.when(t == 2)
        def _():
            event(0, 1)
            event(0, 2)

        @pl.when(t == 6)
        def _():
            event(0, 3)

        nb = order(t)

        def against(i, carry):
            b = order(i)
            stats(jnp.maximum(nb, b), jnp.minimum(nb, b), False)
            return carry

        lax.fori_loop(0, t, against, 0)
        stats(nb, nb, True)
        return carry

    lse[...] = jnp.full_like(lse, jnp.finfo(F32).min)
    lax.fori_loop(0, n, land, 0)

    def pipelined(nb, start, work):
        start(0, 0)

        def pair(p, carry):
            start(2 * p + 1, 1)
            work(2 * p, 0, False)
            start(2 * p + 2, 0)
            work(2 * p + 1, 1, False)
            return carry

        lax.fori_loop(0, nb // 2, pair, 0)

        @pl.when(lax.rem(nb, 2) == 0)
        def _():
            work(nb, 0, True)

        @pl.when(lax.rem(nb, 2) == 1)
        def _():
            start(nb, 1)
            work(nb - 1, 0, False)
            work(nb, 1, True)

    def forward(nb, carry):
        peak = lse[nb]
        top = jnp.max(peak, axis=1, keepdims=True)
        total = jnp.sum(sums(nb) * expo(peak, top), axis=1, keepdims=True)
        lse[nb] = jnp.broadcast_to(top + jnp.log(total) * (1.0 / scale), (blk, lanes))
        oacc[...] = jnp.zeros_like(oacc)

        def start(j, slot):
            s_ref[slot] = _mm_t(q[nb], k[j])

        def values(j, slot, mask):
            shift = lse[nb]
            pr = [expo(part, shift) for part in groups(s_ref[slot])]
            if mask:
                pr = [jnp.where(kg, part, 0.0) for kg, part in zip(groups(keep), pr)]
            oacc[...] += _mm(jnp.concatenate([part.astype(BF16) for part in pr], axis=1), v[j])

        pipelined(nb, start, values)
        o[nb] = oacc[...].astype(BF16)
        return carry

    lax.fori_loop(0, n, forward, 0)

    def q_step(t, carry):
        nb = order(t)

        @pl.when(t == 0)
        def _():
            first(1)
            event(1, 1)

        @pl.when(t == 2)
        def _():
            event(1, 2)

        @pl.when(t == 6)
        def _():
            event(1, 3)
            wevent(1)

        qt[...] = q[nb].T
        dot_[...] = do[nb].T
        delta = jnp.sum(do[nb].astype(F32) * o[nb].astype(F32), axis=1, keepdims=True)
        mrow[...] = jnp.broadcast_to(delta, mrow.shape)
        oacc[...] = jnp.zeros_like(oacc)

        def start(j, slot):
            s_ref[slot] = _mm_t(q[nb], k[j])
            s_ref[2 + slot] = _mm_t(do[nb], v[j])

        def grads(j, slot, mask):
            sc = groups(s_ref[slot])
            dp = groups(s_ref[2 + slot])
            shift, less = lse[nb], mrow[...]
            pr = [expo(part, shift) for part in sc]
            if mask:
                pr = [jnp.where(kg, part, 0.0) for kg, part in zip(groups(keep), pr)]
            ds = jnp.concatenate([(pp * (dd - less)).astype(BF16) for pp, dd in zip(pr, dp)], axis=1)
            pb = jnp.concatenate([pp.astype(BF16) for pp in pr], axis=1)
            oacc[...] += _mm(ds, k[j])
            acc[0, j] += _mm(qt[...], ds)
            acc[1, j] += _mm(dot_[...], pb)

        pipelined(nb, start, grads)
        dq = (oacc[...] * scale).astype(BF16)
        q[nb] = dq
        lhs[nb, 0:width] = dq.T

        @pl.when(t > 0)
        def _():
            _remote(q.at[nb], dqr.at[me], dq_send.at[nb], dq_recv.at[me], nb).start()

        @pl.when(t == 0)
        def _():
            dqr[me] = dq

        return carry

    lax.fori_loop(0, n, q_step, 0)

    f_mine = jnp.where(core == 0, scale, 1.0).astype(F32)
    f_other = jnp.where(core == 0, 1.0, scale).astype(F32)

    def kv_copy(b):
        return _remote(p_ref.at[b, pl.ds(0, width)], lhs.at[b, pl.ds(2 * width, width)],
                       kv_send.at[b], kv_recv.at[b], mate)

    def convert(i, _):
        b = lax.rem(me - core + n // 2 + i, n)
        p_ref[b, 0:width] = (acc[1 - core, b] * f_other).astype(BF16)
        kv_copy(b).start()
        lhs[b, width:2 * width] = (acc[core, b] * f_mine).astype(BF16)
        return _

    lax.fori_loop(0, n, convert, 0)

    half_chips = n // 2

    def stag(b):
        return s_ref.at[half_chips + b // 2, pl.ds(lax.rem(b, 2) * width, width)]

    def pair(b):
        kv_copy(b).wait_recv()
        stag(b)[...] = (lhs[b, width:2 * width].astype(F32)
                        + lhs[b, 2 * width:3 * width].astype(F32))

    base = 2 * chip
    ob_, rb, lb = opp - core, right - core, left - core

    def rs_copy(src, dst, r, side, kind):
        return _remote(src, dst.at[side, kind], rs_send.at[r, side, kind],
                       rs_recv.at[r, side, kind], right if side == 0 else left)

    def rs_start(*args):
        c = rs_copy(*args)
        c.start()
        sends.append(c)

    def rs_wait(dst, r, side, kind):
        rs_copy(dst.at[side, kind], dst, r, side, kind).wait_recv()

    pair(ob_)
    rs_start(stag(ob_), kvr, 0, 0, 0)
    pair(ob_ + 1)
    rs_start(stag(ob_ + 1), kvr, 0, 1, 0)
    pair(rb + 1)
    rs_start(stag(rb + 1), kvr, 0, 0, 2)
    pair(lb)
    rs_start(stag(lb), kvr, 0, 1, 2)
    for b in (rb, lb + 1, base, base + 1):
        pair(b)

    def x_copy(b, slot):
        return pltpu.make_async_copy(xf.at[b], xbuf.at[slot], x_sem.at[slot])

    pltpu.make_async_copy(x, xbuf.at[0], x_sem.at[0]).start()
    wevent(2)

    def x_step(i, carry):
        slot = lax.rem(i, 2)
        b = lax.rem(me + i, n)
        x_copy(b, slot).wait()

        @pl.when(i < n - 1)
        def _():
            x_copy(lax.rem(me + i + 1, n), 1 - slot).start()

        for c in range(model // tile):
            xt = xbuf[slot, :, c * tile:(c + 1) * tile]
            acc[0, c] += _mm(lhs[b, 0:width], xt)
            acc[1, c] += _mm(lhs[b, width:2 * width], xt) + _mm(lhs[b, 2 * width:3 * width], xt)
        return carry

    def clear(c, _):
        acc[0, c] = jnp.zeros_like(acc[0, c])
        acc[1, c] = jnp.zeros_like(acc[1, c])
        return _

    lax.fori_loop(0, half_chips, clear, 0)
    lax.fori_loop(0, n, x_step, 0)
    wevent(3)

    rs_wait(kvr, 0, 0, 0)
    stag(rb)[...] += kvr[0, 0]
    rs_start(stag(rb), kvr, 0, 0, 1)
    rs_wait(kvr, 0, 1, 0)
    stag(lb + 1)[...] += kvr[1, 0]
    rs_start(stag(lb + 1), kvr, 0, 1, 1)

    def part(b):
        return acc.at[1, b // 2, :, pl.ds(lax.rem(b, 2) * (tile // 2), tile // 2)]

    def part_cols(h):
        return slice(h * (tile // 2), (h + 1) * (tile // 2))

    rs_start(acc.at[1, ob_ // 2, :, pl.ds(0, tile // 2)], dwr, 1, 0, 0)
    rs_start(acc.at[1, ob_ // 2, :, pl.ds(tile // 2, tile // 2)], dwr, 1, 1, 0)
    rs_start(acc.at[1, rb // 2, :, pl.ds(tile // 2, tile // 2)], dwr, 1, 0, 2)
    rs_start(acc.at[1, lb // 2, :, pl.ds(0, tile // 2)], dwr, 1, 1, 2)

    def y_copy(b, slot):
        return pltpu.make_async_copy(dyf.at[b], xbuf.at[slot], x_sem.at[slot])

    pltpu.make_async_copy(dy, xbuf.at[0], x_sem.at[0]).start()
    part_w = model // n
    dwo_v[...] = jnp.zeros_like(dwo_v)

    def y_step(i, carry):
        slot = lax.rem(i, 2)
        b = lax.rem(me + i, n)
        ot = o[b].T
        y_copy(b, slot).wait()

        @pl.when(i < n - 1)
        def _():
            y_copy(lax.rem(me + i + 1, n), 1 - slot).start()

        for c in range(n):
            dwo_v[c] += _mm(ot, xbuf[slot, :, c * part_w:(c + 1) * part_w])
        return carry

    lax.fori_loop(0, n, y_step, 0)
    outs = [pltpu.make_async_copy(dwo_v.at[c], dwo.at[:, pl.ds(c * part_w, part_w)], y_sem.at[c])
            for c in range(n)]
    for c in outs:
        c.start()

    for b in range(n):
        kv_copy(b).wait_send()
    wtwin()
    for b in (mate, left + flip, right + flip, opp + flip):
        for i in range(4):
            wrecv(b, i)
    for d in range(1, n):
        peer = lax.rem(me + d, n)
        _remote(dqr.at[peer], dqr.at[peer], dq_send.at[peer], dq_recv.at[peer], peer).wait_recv()

    def w_copy(h, c, slot):
        return pltpu.make_async_copy(wqf.at[h, pl.ds(c * tile, tile)],
                                     p_ref.at[h, :, pl.ds(slot * width, width)], b_sem.at[slot, h])

    def own_copy(c, slot):
        return pltpu.make_async_copy(wq.at[pl.ds(c * tile, tile)],
                                     p_ref.at[me, :, pl.ds(slot * width, width)], b_sem.at[slot, me])

    def w_load(c, slot):
        own_copy(c, slot).start()
        for d in range(1, n):
            w_copy(lax.rem(me + d, n), c, slot).start()

    w_load(0, 0)
    for c in range(model // tile):
        slot = c % 2
        for h in range(n):
            w_copy(h, c, slot).wait()
        if c + 1 < model // tile:
            w_load(c + 1, 1 - slot)
        s_ref[c] = jnp.zeros_like(s_ref[c])

        def heads(h, _):
            s_ref[c] += _mm_t(dqr[h], p_ref[h, :, slot * width:(slot + 1) * width])
            return _

        lax.fori_loop(0, n, heads, 0)

    def q_copy(c):
        return pltpu.make_async_copy(lse.at[pl.ds(2 * c, 2)], dwq.at[pl.ds(2 * c, 2)], l_sem.at[c])

    for c in range(model // tile):
        for g in range(4):
            lse[2 * c + g // 2, pl.ds(g % 2, half, stride=2)] = (
                acc[0, c, (g % 2) * lanes:(g % 2 + 1) * lanes, (g // 2) * half:(g // 2 + 1) * half].T)
        q_copy(c).start()

    rs_wait(kvr, 0, 0, 1)
    rs_wait(kvr, 0, 1, 2)
    stag(base)[...] += kvr[0, 1] + kvr[1, 2]
    rs_wait(kvr, 0, 0, 2)
    rs_wait(kvr, 0, 1, 1)
    stag(base + 1)[...] += kvr[0, 2] + kvr[1, 1]
    swap = _remote(stag(mate), kvx.at[0], b_sem.at[2, 0], b_sem.at[2, 1], mate)
    swap.start()
    kvx[1] = stag(me)[...]

    rs_wait(dwr, 1, 0, 0)
    acc[1, rb // 2, :, part_cols(0)] += dwr[0, 0]
    rs_start(acc.at[1, rb // 2, :, pl.ds(0, tile // 2)], dwr, 1, 0, 1)
    rs_wait(dwr, 1, 1, 0)
    acc[1, lb // 2, :, part_cols(1)] += dwr[1, 0]
    rs_start(acc.at[1, lb // 2, :, pl.ds(tile // 2, tile // 2)], dwr, 1, 1, 1)

    swap.wait()
    kv_first = kvx[1 - core].T
    kv_second = kvx[core].T

    def split(val):
        hi = val.astype(BF16)
        rest = val - hi.astype(F32)
        mid = rest.astype(BF16)
        lo = (rest - mid.astype(F32)).astype(BF16)
        return hi, mid, lo

    for d in range(1, n):
        peer = lax.rem(me + d, n)
        _remote(dqr.at[peer], dqr.at[peer], dq_send.at[peer], dq_recv.at[peer], peer).wait_send()
    for i, parts in enumerate((split(kv_first), split(kv_second))):
        for g, val in enumerate(parts):
            q[3 * i + g] = val
    for c in range(model // tile):
        at = slice(c * tile, (c + 1) * tile)
        total = s_ref[c]
        for i, w in enumerate((wk_v, wv_v)):
            wt = w[at]
            total += (_mm_t(q[3 * i + 2], wt) + _mm_t(q[3 * i + 1], wt)) + _mm_t(q[3 * i], wt)
        xbuf[0, :, at] = total.astype(BF16)
    out_dx = pltpu.make_async_copy(xbuf.at[0], dx, x_sem.at[0])
    out_dx.start()

    outs.append(out_dx)
    rs_wait(dwr, 1, 0, 1)
    rs_wait(dwr, 1, 1, 2)
    acc[1, base // 2, :, part_cols(0)] += dwr[0, 1] + dwr[1, 2]
    rs_wait(dwr, 1, 0, 2)
    rs_wait(dwr, 1, 1, 1)
    acc[1, base // 2, :, part_cols(1)] += dwr[0, 2] + dwr[1, 1]
    swap = _remote(part(mate), dwx.at[0], b_sem.at[2, 2], b_sem.at[2, 3], mate)
    swap.start()
    dwx[1] = part(me)[...]
    swap.wait()
    for i, (val, out) in enumerate(((dwx[1 - core].T, dwk), (dwx[core].T, dwv))):
        oacc[i * width:(i + 1) * width] = val
        outs.append(pltpu.make_async_copy(oacc.at[pl.ds(i * width, width)], out, o_sem.at[1 + i]))
        outs[-1].start()
    for c in outs:
        c.wait()
    for c in range(model // tile):
        q_copy(c).wait()

    for c in sends:
        c.wait_send()
    for a in range(2):
        for i in range(3):
            _remote(view(a, me, 0), view(a, me, 0), g_sr.at[a, i], g_recv.at[a, 0], mate).wait_send()
            _remote(view(a, me, 0), view(a, me, 0), g_sl.at[a, i], g_recv.at[a, 0], mate).wait_send()
        for i in range(8):
            _remote(view(a, me, 0), view(a, me, 0), g_sp.at[a, i], g_recv.at[a, 0], mate).wait_send()
    for sems, count in ((w_sr, 3), (w_sl, 3), (w_sp, 16), (w_st, 6)):
        for i in range(count):
            wcopy(wview(me, 0), me, 0, sems.at[i], mate).wait_send()


def solution(mesh):
    n = mesh.shape["tp"]
    hbm = pl.BlockSpec(memory_space=pl.ANY)
    dma = pltpu.SemaphoreType.DMA

    def local_grads(x_blk, dy_blk, wq_loc, w_k, w_v, wo_loc):
        model, kv_heads, width = w_k.shape
        rows = x_blk.shape[0]
        scale = width ** -0.5
        wq2 = wq_loc.reshape(model, width)
        wk2 = w_k.reshape(model, width)
        wv2 = w_v.reshape(model, width)
        wo2 = wo_loc.reshape(width, model)
        tile = 2 * model // n
        full = jax.ShapeDtypeStruct((n, rows, model), BF16)
        proj = pltpu.VMEM((n, rows, width), BF16)
        dx, dwq, dwo, dwk, dwv, _, _, _ = pl.pallas_call(
            functools.partial(_kernel, n, scale),
            name="attention_grads",
            out_shape=(
                jax.ShapeDtypeStruct((rows, model), BF16),
                jax.ShapeDtypeStruct((n, rows, 128), F32),
                jax.ShapeDtypeStruct((width, model), F32),
                jax.ShapeDtypeStruct((model // n, width), F32),
                jax.ShapeDtypeStruct((model // n, width), F32),
                full, full,
                jax.ShapeDtypeStruct((n, model, width), BF16),
            ),
            in_specs=[hbm] * 6,
            out_specs=(hbm,) * 8,
            scratch_shapes=[
                proj, proj, proj, proj,
                pltpu.VMEM((model, width), BF16),
                pltpu.VMEM((model, width), BF16),
                pltpu.VMEM((model, width), BF16),
                pltpu.VMEM((width, model), BF16),
                pltpu.VMEM((n, rows, rows), F32),
                pltpu.VMEM((n, rows, rows), BF16),
                pltpu.VMEM((2, n, width, rows), F32),
                pltpu.VMEM((n, 3 * width, rows), BF16),
                pltpu.VMEM((n, rows, width), BF16),
                pltpu.VMEM((n, rows, 128), F32),
                pltpu.VMEM((n, rows, width), BF16),
                pltpu.VMEM((2, 3, width, rows), F32),
                pltpu.VMEM((2, width, rows), F32),
                pltpu.VMEM((2, 3, width, tile // 2), F32),
                pltpu.VMEM((2, width, tile // 2), F32),
                pltpu.VMEM((2, rows, model), BF16),
                pltpu.VMEM((rows, 128), F32),
                pltpu.VMEM((rows, width), F32),
                pltpu.VMEM((width, rows), BF16),
                pltpu.VMEM((width, rows), BF16),
                pltpu.VMEM((n, rows // 2, model // n), F32),
                dma((2, 3)), dma((2, 3)), dma((2, 8)), dma((2, 2 * n)), dma((4,)),
                dma((3,)), dma((3,)), dma((16,)), dma((6,)), dma((n, 4)),
                dma((n,)), dma((n,)), dma((n,)), dma((n,)),
                dma((2, 2, 3)), dma((2, 2, 3)), dma((2,)), dma((3, n)), dma((4,)), dma((n,)),
            ],
            compiler_params=pltpu.CompilerParams(
                collective_id=0, has_side_effects=True, vmem_limit_bytes=VMEM_MAX),
        )(x_blk, dy_blk, wq2, wk2, wv2, wo2)
        return (dx, dwq.reshape(model, 1, width), dwo.reshape(1, width, model), dwk, dwv)

    tok_spec = P(("dp", "tp"))
    return jax.shard_map(
        local_grads,
        mesh=mesh,
        in_specs=(tok_spec, tok_spec, P(None, "tp", None), P(), P(), P("tp")),
        out_specs=(tok_spec, P("dp", "tp", None), tok_spec, tok_spec, tok_spec),
        check_vma=False,
    )
```

```python
import functools

import jax
import jax.numpy as jnp
from jax import lax
from jax.experimental import pallas as pl
from jax.experimental.pallas import tpu as pltpu
from jax.sharding import PartitionSpec as P

MESH = pl.DeviceIdType.MESH
F32 = jnp.float32
BF16 = jnp.bfloat16
LOG2E = 1.4426950408889634
VMEM_MAX = 67_043_328


def _mm(a, b):
    return lax.dot_general(a, b, (((1,), (0,)), ((), ())), preferred_element_type=F32)


def _mm_t(a, b):
    return lax.dot_general(a, b, (((1,), (1,)), ((), ())), preferred_element_type=F32)


def _ring(n):
    me = lax.axis_index("tp")
    core = lax.rem(me, 2)
    right = lax.rem(me + 2, n)
    left = lax.rem(me + n - 2, n)
    opp = lax.rem(me + n // 2, n)
    mate = me + 1 - 2 * core
    return me, core, right, left, opp, mate


def _barrier(devices):
    barrier = pltpu.get_barrier_semaphore()
    for d in devices:
        pl.semaphore_signal(barrier, inc=1, device_id=d, device_id_type=MESH)
    pl.semaphore_wait(barrier, len(devices))


def _remote(src, dst, ssem, rsem, dev):
    return pltpu.make_async_remote_copy(
        src_ref=src, dst_ref=dst, send_sem=ssem, recv_sem=rsem,
        device_id={"tp": dev}, device_id_type=MESH)


def _kernel(n, scale, x, dy, wq, wk, wv, wo,
            dx, dwq, dwo, dwk, dwv, xf, dyf, wqf,
            q, k, v, do, wq_v, wk_v, wv_v, wo_v,
            s_ref, p_ref, acc, lhs, o, lse, dqr, kvr, kvx, dwr, dwx, xbuf,
            mrow, oacc, qt, dot_, dwo_v,
            g_sr, g_sl, g_sp, g_recv, l_sem,
            w_sr, w_sl, w_sp, w_st, w_recv, dq_send, dq_recv, kv_send, kv_recv,
            rs_send, rs_recv, x_sem, b_sem, o_sem, y_sem):
    me, core, right, left, opp, mate = _ring(n)
    chip = me // 2
    flip = 1 - 2 * core
    blk, width = q.shape[1], q.shape[2]
    half = blk // 2
    model = x.shape[1]
    tile = model // (n // 2)
    lanes = 128
    group = lax.axis_index("dp")
    side = lax.rem(group, 2)
    twin = {"dp": group + 1 - 2 * side, "tp": me}
    _barrier([{"tp": lax.rem(me + d, n)} for d in range(1, n)] + [twin])
    sends = []

    srcs, dsts = (x, dy), (xf, dyf)

    def view(a, b, h):
        return dsts[a].at[b, pl.ds(h * half, half)]

    def send(src, a, b, h, ssem, dev):
        _remote(src, view(a, b, h), ssem, g_recv.at[a, b * 2 + h], dev).start()

    def recv(a, b, h):
        _remote(view(a, b, h), view(a, b, h), g_sp.at[a, 0], g_recv.at[a, b * 2 + h], mate).wait_recv()

    def own(a, h):
        return srcs[a].at[pl.ds(h * half, half)]

    def send_own(a):
        for i, h in enumerate((0, 1)):
            send(own(a, h), a, me, h, g_sr.at[a, i], right)
            send(own(a, 1 - h), a, me, 1 - h, g_sl.at[a, i], left)

    def chunk(i):
        return xbuf.at[i // 2, pl.ds(lax.rem(i, 2) * half, half)]

    def load(src, i):
        return pltpu.make_async_copy(src, chunk(i), l_sem.at[i])

    def project(a, b0, h0, b1, h1):
        def body(i, carry):
            side, par = lax.rem(i, 2), i // 2
            b = b0 + side * (b1 - b0) + par * flip
            h = h0 + side * (h1 - h0)
            load(view(a, b, h), i).wait()
            at = pl.ds(pl.multiple_of(h * half, half), half)
            data = chunk(i)[...]
            if a == 0:
                q[b, at] = _mm(data, wq_v[...]).astype(BF16)
                k[b, at] = _mm(data, wk_v[...]).astype(BF16)
                v[b, at] = _mm(data, wv_v[...]).astype(BF16)
            else:
                do[b, at] = _mm_t(data, wo_v[...]).astype(BF16)
            return carry
        lax.fori_loop(0, 4, body, 0)

    def first(a):
        for h in range(2):
            load(own(a, h), h).start()
        for h in range(2):
            recv(a, mate, h)
            load(view(a, mate, h), 2 + h).start()
        project(a, me, 0, me, 1)

    def event(a, e):
        b0, h0, b1, h1 = ((left, 0, right, 1), (left, 1, right, 0), (opp, 0, opp, 1))[e - 1]
        for i, (b, h) in enumerate(((b0, h0), (b1, h1))):
            recv(a, b, h)
            if e == 1:
                send(view(a, b, h), a, b, h, (g_sr, g_sl)[i].at[a, 2], (right, left)[i])
            send(view(a, b, h), a, b, h, g_sp.at[a, 2 * e + i], mate)
            load(view(a, b, h), i).start()
        if e == 1:
            if a == 0:
                send_own(1)
            else:
                send_wq()
        for i, (b, h) in enumerate(((b0, h0), (b1, h1))):
            recv(a, b + flip, h)
            load(view(a, b + flip, h), 2 + i).start()
        project(a, b0, h0, b1, h1)

    quarter = model // 4

    def wview(b, i):
        return wqf.at[b, pl.ds(i * quarter, quarter)]

    def wcopy(src, b, i, ssem, dev):
        dev = dev if isinstance(dev, dict) else {"tp": dev}
        return pltpu.make_async_remote_copy(
            src_ref=src, dst_ref=wview(b, i), send_sem=ssem, recv_sem=w_recv.at[b, i],
            device_id=dev, device_id_type=MESH)

    def wrecv(b, i):
        wcopy(wview(b, i), b, i, w_sp.at[0], mate).wait_recv()

    def wown(i):
        return wq.at[pl.ds(i * quarter, quarter)]

    mine, other = 2 * side, 2 - 2 * side

    def send_wq():
        for i in range(2):
            for g, sems, dev in ((i, w_sr, right), (1 - i, w_sl, left)):
                src = wq_v.at[pl.ds((mine + g) * quarter, quarter)]
                wcopy(src, me, mine + g, sems.at[i], dev).start()

    def wevent(e):
        pieces = (((left, 0), (right, 1)), ((left, 1), (right, 0)), ((opp, 0), (opp, 1)))[e - 1]
        for g, (b, i) in enumerate(pieces):
            i = mine + i
            wrecv(b, i)
            if e == 1:
                wcopy(wview(b, i), b, i, (w_sr, w_sl)[g].at[2], (right, left)[g]).start()
            wcopy(wview(b, i), b, i, w_sp.at[2 + 2 * e + g], mate).start()
            wcopy(wview(b, i), b, i, w_st.at[2 * e - 2 + g], twin).start()

    def wtwin():
        for g, (b, i) in enumerate(((left, 0), (right, 1), (left, 1), (right, 0), (opp, 0), (opp, 1))):
            i = other + i
            wrecv(b, i)
            wcopy(wview(b, i), b, i, w_sp.at[10 + g], mate).start()

    send_own(0)
    for a in range(2):
        for h in range(2):
            send(own(a, h), a, me, h, g_sp.at[a, h], mate)
    for i in range(4):
        wcopy(wown(i), me, i, w_sp.at[i], mate).start()
    loads = [pltpu.make_async_copy(src, dst, o_sem.at[i])
             for i, (src, dst) in enumerate(((wq, wq_v), (wk, wk_v), (wv, wv_v), (wo, wo_v)))]
    for c in loads:
        c.start()
    acc[...] = jnp.zeros_like(acc)
    dwo_v[...] = jnp.zeros_like(dwo_v)
    for c in loads:
        c.wait()

    def fold(val, op):
        out = val[:, :lanes]
        for c in range(1, val.shape[1] // lanes):
            out = op(out, val[:, c * lanes:(c + 1) * lanes])
        return out

    def groups(val):
        return [val[:, c * lanes:(c + 1) * lanes] for c in range(val.shape[1] // lanes)]

    def expo(val, top):
        return jnp.exp2((val - top) * (scale * LOG2E))

    keep = (lax.broadcasted_iota(jnp.int32, (blk, blk), 0)
            >= lax.broadcasted_iota(jnp.int32, (blk, blk), 1))

    def order(t):
        p = t // 2
        return lax.rem(me + 2 * p + 2 * (p // 2) * (1 - 2 * lax.rem(p, 2)), n) + lax.rem(t, 2) * flip

    def sums(nb):
        return jnp.concatenate([dwo_v[nb, :, 0:lanes], dwo_v[nb, :, lanes:2 * lanes]], axis=0)

    def stats(nb, j, mask):
        sc = _mm_t(q[nb], k[j])
        if mask:
            sc = jnp.where(keep, sc, -jnp.inf)
        old = lse[nb]
        top = jnp.maximum(old, fold(sc, jnp.maximum))
        total = sums(nb) * expo(old, top)
        for part in groups(sc):
            total += expo(part, top)
        lse[nb] = top
        dwo_v[nb, :, 0:lanes] = total[:half]
        dwo_v[nb, :, lanes:2 * lanes] = total[half:]

    def land(t, carry):
        @pl.when(t == 0)
        def _():
            first(0)

        @pl.when(t == 2)
        def _():
            event(0, 1)
            event(0, 2)

        @pl.when(t == 6)
        def _():
            event(0, 3)

        nb = order(t)

        def against(i, carry):
            b = order(i)
            stats(jnp.maximum(nb, b), jnp.minimum(nb, b), False)
            return carry

        lax.fori_loop(0, t, against, 0)
        stats(nb, nb, True)
        return carry

    lse[...] = jnp.full_like(lse, jnp.finfo(F32).min)
    lax.fori_loop(0, n, land, 0)

    def pipelined(nb, start, work):
        start(0, 0)

        def pair(p, carry):
            start(2 * p + 1, 1)
            work(2 * p, 0, False)
            start(2 * p + 2, 0)
            work(2 * p + 1, 1, False)
            return carry

        lax.fori_loop(0, nb // 2, pair, 0)

        @pl.when(lax.rem(nb, 2) == 0)
        def _():
            work(nb, 0, True)

        @pl.when(lax.rem(nb, 2) == 1)
        def _():
            start(nb, 1)
            work(nb - 1, 0, False)
            work(nb, 1, True)

    def forward(nb, carry):
        peak = lse[nb]
        top = jnp.max(peak, axis=1, keepdims=True)
        total = jnp.sum(sums(nb) * expo(peak, top), axis=1, keepdims=True)
        lse[nb] = jnp.broadcast_to(top + jnp.log(total) * (1.0 / scale), (blk, lanes))
        oacc[...] = jnp.zeros_like(oacc)

        def start(j, slot):
            s_ref[slot] = _mm_t(q[nb], k[j])

        def values(j, slot, mask):
            shift = lse[nb]
            pr = [expo(part, shift) for part in groups(s_ref[slot])]
            if mask:
                pr = [jnp.where(kg, part, 0.0) for kg, part in zip(groups(keep), pr)]
            oacc[...] += _mm(jnp.concatenate([part.astype(BF16) for part in pr], axis=1), v[j])

        pipelined(nb, start, values)
        o[nb] = oacc[...].astype(BF16)
        return carry

    lax.fori_loop(0, n, forward, 0)

    def q_step(t, carry):
        nb = order(t)

        @pl.when(t == 0)
        def _():
            first(1)
            event(1, 1)

        @pl.when(t == 2)
        def _():
            event(1, 2)

        @pl.when(t == 6)
        def _():
            event(1, 3)
            wevent(1)

        qt[...] = q[nb].T
        dot_[...] = do[nb].T
        delta = jnp.sum(do[nb].astype(F32) * o[nb].astype(F32), axis=1, keepdims=True)
        mrow[...] = jnp.broadcast_to(delta, mrow.shape)
        oacc[...] = jnp.zeros_like(oacc)

        def start(j, slot):
            s_ref[slot] = _mm_t(q[nb], k[j])
            s_ref[2 + slot] = _mm_t(do[nb], v[j])

        def grads(j, slot, mask):
            sc = groups(s_ref[slot])
            dp = groups(s_ref[2 + slot])
            shift, less = lse[nb], mrow[...]
            pr = [expo(part, shift) for part in sc]
            if mask:
                pr = [jnp.where(kg, part, 0.0) for kg, part in zip(groups(keep), pr)]
            ds = jnp.concatenate([(pp * (dd - less)).astype(BF16) for pp, dd in zip(pr, dp)], axis=1)
            pb = jnp.concatenate([pp.astype(BF16) for pp in pr], axis=1)
            oacc[...] += _mm(ds, k[j])
            acc[0, j] += _mm(qt[...], ds)
            acc[1, j] += _mm(dot_[...], pb)

        pipelined(nb, start, grads)
        dq = (oacc[...] * scale).astype(BF16)
        q[nb] = dq
        lhs[nb, 0:width] = dq.T

        @pl.when(t > 0)
        def _():
            _remote(q.at[nb], dqr.at[me], dq_send.at[nb], dq_recv.at[me], nb).start()

        @pl.when(t == 0)
        def _():
            dqr[me] = dq

        return carry

    lax.fori_loop(0, n, q_step, 0)

    f_mine = jnp.where(core == 0, scale, 1.0).astype(F32)
    f_other = jnp.where(core == 0, 1.0, scale).astype(F32)

    def kv_copy(b):
        return _remote(p_ref.at[b, pl.ds(0, width)], lhs.at[b, pl.ds(2 * width, width)],
                       kv_send.at[b], kv_recv.at[b], mate)

    def convert(i, _):
        b = lax.rem(me - core + n // 2 + i, n)
        p_ref[b, 0:width] = (acc[1 - core, b] * f_other).astype(BF16)
        kv_copy(b).start()
        lhs[b, width:2 * width] = (acc[core, b] * f_mine).astype(BF16)
        return _

    lax.fori_loop(0, n, convert, 0)

    half_chips = n // 2

    def stag(b):
        return s_ref.at[half_chips + b // 2, pl.ds(lax.rem(b, 2) * width, width)]

    def pair(b):
        kv_copy(b).wait_recv()
        stag(b)[...] = (lhs[b, width:2 * width].astype(F32)
                        + lhs[b, 2 * width:3 * width].astype(F32))

    base = 2 * chip
    ob_, rb, lb = opp - core, right - core, left - core

    def rs_copy(src, dst, r, side, kind):
        return _remote(src, dst.at[side, kind], rs_send.at[r, side, kind],
                       rs_recv.at[r, side, kind], right if side == 0 else left)

    def rs_start(*args):
        c = rs_copy(*args)
        c.start()
        sends.append(c)

    def rs_wait(dst, r, side, kind):
        rs_copy(dst.at[side, kind], dst, r, side, kind).wait_recv()

    pair(ob_)
    rs_start(stag(ob_), kvr, 0, 0, 0)
    pair(ob_ + 1)
    rs_start(stag(ob_ + 1), kvr, 0, 1, 0)
    pair(rb + 1)
    rs_start(stag(rb + 1), kvr, 0, 0, 2)
    pair(lb)
    rs_start(stag(lb), kvr, 0, 1, 2)
    for b in (rb, lb + 1, base, base + 1):
        pair(b)

    def x_copy(b, slot):
        return pltpu.make_async_copy(xf.at[b], xbuf.at[slot], x_sem.at[slot])

    pltpu.make_async_copy(x, xbuf.at[0], x_sem.at[0]).start()
    wevent(2)

    def x_step(i, carry):
        slot = lax.rem(i, 2)
        b = lax.rem(me + i, n)
        x_copy(b, slot).wait()

        @pl.when(i < n - 1)
        def _():
            x_copy(lax.rem(me + i + 1, n), 1 - slot).start()

        for c in range(model // tile):
            xt = xbuf[slot, :, c * tile:(c + 1) * tile]
            acc[0, c] += _mm(lhs[b, 0:width], xt)
            acc[1, c] += _mm(lhs[b, width:2 * width], xt) + _mm(lhs[b, 2 * width:3 * width], xt)
        return carry

    def clear(c, _):
        acc[0, c] = jnp.zeros_like(acc[0, c])
        acc[1, c] = jnp.zeros_like(acc[1, c])
        return _

    lax.fori_loop(0, half_chips, clear, 0)
    lax.fori_loop(0, n, x_step, 0)
    wevent(3)

    rs_wait(kvr, 0, 0, 0)
    stag(rb)[...] += kvr[0, 0]
    rs_start(stag(rb), kvr, 0, 0, 1)
    rs_wait(kvr, 0, 1, 0)
    stag(lb + 1)[...] += kvr[1, 0]
    rs_start(stag(lb + 1), kvr, 0, 1, 1)

    def part(b):
        return acc.at[1, b // 2, :, pl.ds(lax.rem(b, 2) * (tile // 2), tile // 2)]

    def part_cols(h):
        return slice(h * (tile // 2), (h + 1) * (tile // 2))

    rs_start(acc.at[1, ob_ // 2, :, pl.ds(0, tile // 2)], dwr, 1, 0, 0)
    rs_start(acc.at[1, ob_ // 2, :, pl.ds(tile // 2, tile // 2)], dwr, 1, 1, 0)
    rs_start(acc.at[1, rb // 2, :, pl.ds(tile // 2, tile // 2)], dwr, 1, 0, 2)
    rs_start(acc.at[1, lb // 2, :, pl.ds(0, tile // 2)], dwr, 1, 1, 2)

    def y_copy(b, slot):
        return pltpu.make_async_copy(dyf.at[b], xbuf.at[slot], x_sem.at[slot])

    pltpu.make_async_copy(dy, xbuf.at[0], x_sem.at[0]).start()
    part_w = model // n
    dwo_v[...] = jnp.zeros_like(dwo_v)

    def y_step(i, carry):
        slot = lax.rem(i, 2)
        b = lax.rem(me + i, n)
        ot = o[b].T
        y_copy(b, slot).wait()

        @pl.when(i < n - 1)
        def _():
            y_copy(lax.rem(me + i + 1, n), 1 - slot).start()

        for c in range(n):
            dwo_v[c] += _mm(ot, xbuf[slot, :, c * part_w:(c + 1) * part_w])
        return carry

    lax.fori_loop(0, n, y_step, 0)
    outs = [pltpu.make_async_copy(dwo_v.at[c], dwo.at[:, pl.ds(c * part_w, part_w)], y_sem.at[c])
            for c in range(n)]
    for c in outs:
        c.start()

    for b in range(n):
        kv_copy(b).wait_send()
    wtwin()
    for b in (mate, left + flip, right + flip, opp + flip):
        for i in range(4):
            wrecv(b, i)
    for d in range(1, n):
        peer = lax.rem(me + d, n)
        _remote(dqr.at[peer], dqr.at[peer], dq_send.at[peer], dq_recv.at[peer], peer).wait_recv()

    def w_copy(h, c, slot):
        return pltpu.make_async_copy(wqf.at[h, pl.ds(c * tile, tile)],
                                     p_ref.at[h, :, pl.ds(slot * width, width)], b_sem.at[slot, h])

    def own_copy(c, slot):
        return pltpu.make_async_copy(wq.at[pl.ds(c * tile, tile)],
                                     p_ref.at[me, :, pl.ds(slot * width, width)], b_sem.at[slot, me])

    def w_load(c, slot):
        own_copy(c, slot).start()
        for d in range(1, n):
            w_copy(lax.rem(me + d, n), c, slot).start()

    w_load(0, 0)
    for c in range(model // tile):
        slot = c % 2
        for h in range(n):
            w_copy(h, c, slot).wait()
        if c + 1 < model // tile:
            w_load(c + 1, 1 - slot)
        s_ref[c] = jnp.zeros_like(s_ref[c])

        def heads(h, _):
            s_ref[c] += _mm_t(dqr[h], p_ref[h, :, slot * width:(slot + 1) * width])
            return _

        lax.fori_loop(0, n, heads, 0)

    def q_copy(c):
        return pltpu.make_async_copy(lse.at[pl.ds(2 * c, 2)], dwq.at[pl.ds(2 * c, 2)], l_sem.at[c])

    for c in range(model // tile):
        for g in range(4):
            lse[2 * c + g // 2, pl.ds(g % 2, half, stride=2)] = (
                acc[0, c, (g % 2) * lanes:(g % 2 + 1) * lanes, (g // 2) * half:(g // 2 + 1) * half].T)
        q_copy(c).start()

    rs_wait(kvr, 0, 0, 1)
    rs_wait(kvr, 0, 1, 2)
    stag(base)[...] += kvr[0, 1] + kvr[1, 2]
    rs_wait(kvr, 0, 0, 2)
    rs_wait(kvr, 0, 1, 1)
    stag(base + 1)[...] += kvr[0, 2] + kvr[1, 1]
    swap = _remote(stag(mate), kvx.at[0], b_sem.at[2, 0], b_sem.at[2, 1], mate)
    swap.start()
    kvx[1] = stag(me)[...]

    rs_wait(dwr, 1, 0, 0)
    acc[1, rb // 2, :, part_cols(0)] += dwr[0, 0]
    rs_start(acc.at[1, rb // 2, :, pl.ds(0, tile // 2)], dwr, 1, 0, 1)
    rs_wait(dwr, 1, 1, 0)
    acc[1, lb // 2, :, part_cols(1)] += dwr[1, 0]
    rs_start(acc.at[1, lb // 2, :, pl.ds(tile // 2, tile // 2)], dwr, 1, 1, 1)

    swap.wait()
    kv_first = kvx[1 - core].T
    kv_second = kvx[core].T

    def split(val):
        hi = val.astype(BF16)
        rest = val - hi.astype(F32)
        mid = rest.astype(BF16)
        lo = (rest - mid.astype(F32)).astype(BF16)
        return hi, mid, lo

    for d in range(1, n):
        peer = lax.rem(me + d, n)
        _remote(dqr.at[peer], dqr.at[peer], dq_send.at[peer], dq_recv.at[peer], peer).wait_send()
    for i, parts in enumerate((split(kv_first), split(kv_second))):
        for g, val in enumerate(parts):
            q[3 * i + g] = val
    for c in range(model // tile):
        at = slice(c * tile, (c + 1) * tile)
        total = s_ref[c]
        for i, w in enumerate((wk_v, wv_v)):
            wt = w[at]
            total += (_mm_t(q[3 * i + 2], wt) + _mm_t(q[3 * i + 1], wt)) + _mm_t(q[3 * i], wt)
        xbuf[0, :, at] = total.astype(BF16)
    out_dx = pltpu.make_async_copy(xbuf.at[0], dx, x_sem.at[0])
    out_dx.start()

    outs.append(out_dx)
    rs_wait(dwr, 1, 0, 1)
    rs_wait(dwr, 1, 1, 2)
    acc[1, base // 2, :, part_cols(0)] += dwr[0, 1] + dwr[1, 2]
    rs_wait(dwr, 1, 0, 2)
    rs_wait(dwr, 1, 1, 1)
    acc[1, base // 2, :, part_cols(1)] += dwr[0, 2] + dwr[1, 1]
    swap = _remote(part(mate), dwx.at[0], b_sem.at[2, 2], b_sem.at[2, 3], mate)
    swap.start()
    dwx[1] = part(me)[...]
    swap.wait()
    for i, (val, out) in enumerate(((dwx[1 - core].T, dwk), (dwx[core].T, dwv))):
        oacc[i * width:(i + 1) * width] = val
        outs.append(pltpu.make_async_copy(oacc.at[pl.ds(i * width, width)], out, o_sem.at[1 + i]))
        outs[-1].start()
    for c in outs:
        c.wait()
    for c in range(model // tile):
        q_copy(c).wait()

    for c in sends:
        c.wait_send()
    for a in range(2):
        for i in range(3):
            _remote(view(a, me, 0), view(a, me, 0), g_sr.at[a, i], g_recv.at[a, 0], mate).wait_send()
            _remote(view(a, me, 0), view(a, me, 0), g_sl.at[a, i], g_recv.at[a, 0], mate).wait_send()
        for i in range(8):
            _remote(view(a, me, 0), view(a, me, 0), g_sp.at[a, i], g_recv.at[a, 0], mate).wait_send()
    for sems, count in ((w_sr, 3), (w_sl, 3), (w_sp, 16), (w_st, 6)):
        for i in range(count):
            wcopy(wview(me, 0), me, 0, sems.at[i], mate).wait_send()


def solution(mesh):
    n = mesh.shape["tp"]
    hbm = pl.BlockSpec(memory_space=pl.ANY)
    dma = pltpu.SemaphoreType.DMA

    def local_grads(x_blk, dy_blk, wq_loc, w_k, w_v, wo_loc):
        model, kv_heads, width = w_k.shape
        rows = x_blk.shape[0]
        scale = width ** -0.5
        wq2 = wq_loc.reshape(model, width)
        wk2 = w_k.reshape(model, width)
        wv2 = w_v.reshape(model, width)
        wo2 = wo_loc.reshape(width, model)
        tile = 2 * model // n
        full = jax.ShapeDtypeStruct((n, rows, model), BF16)
        proj = pltpu.VMEM((n, rows, width), BF16)
        dx, dwq, dwo, dwk, dwv, _, _, _ = pl.pallas_call(
            functools.partial(_kernel, n, scale),
            name="attention_grads",
            out_shape=(
                jax.ShapeDtypeStruct((rows, model), BF16),
                jax.ShapeDtypeStruct((n, rows, 128), F32),
                jax.ShapeDtypeStruct((width, model), F32),
                jax.ShapeDtypeStruct((model // n, width), F32),
                jax.ShapeDtypeStruct((model // n, width), F32),
                full, full,
                jax.ShapeDtypeStruct((n, model, width), BF16),
            ),
            in_specs=[hbm] * 6,
            out_specs=(hbm,) * 8,
            scratch_shapes=[
                proj, proj, proj, proj,
                pltpu.VMEM((model, width), BF16),
                pltpu.VMEM((model, width), BF16),
                pltpu.VMEM((model, width), BF16),
                pltpu.VMEM((width, model), BF16),
                pltpu.VMEM((n, rows, rows), F32),
                pltpu.VMEM((n, rows, rows), BF16),
                pltpu.VMEM((2, n, width, rows), F32),
                pltpu.VMEM((n, 3 * width, rows), BF16),
                pltpu.VMEM((n, rows, width), BF16),
                pltpu.VMEM((n, rows, 128), F32),
                pltpu.VMEM((n, rows, width), BF16),
                pltpu.VMEM((2, 3, width, rows), F32),
                pltpu.VMEM((2, width, rows), F32),
                pltpu.VMEM((2, 3, width, tile // 2), F32),
                pltpu.VMEM((2, width, tile // 2), F32),
                pltpu.VMEM((2, rows, model), BF16),
                pltpu.VMEM((rows, 128), F32),
                pltpu.VMEM((rows, width), F32),
                pltpu.VMEM((width, rows), BF16),
                pltpu.VMEM((width, rows), BF16),
                pltpu.VMEM((n, rows // 2, model // n), F32),
                dma((2, 3)), dma((2, 3)), dma((2, 8)), dma((2, 2 * n)), dma((4,)),
                dma((3,)), dma((3,)), dma((16,)), dma((6,)), dma((n, 4)),
                dma((n,)), dma((n,)), dma((n,)), dma((n,)),
                dma((2, 2, 3)), dma((2, 2, 3)), dma((2,)), dma((3, n)), dma((4,)), dma((n,)),
            ],
            compiler_params=pltpu.CompilerParams(
                collective_id=0, has_side_effects=True, vmem_limit_bytes=VMEM_MAX),
        )(x_blk, dy_blk, wq2, wk2, wv2, wo2)
        return (dx, dwq.reshape(model, 1, width), dwo.reshape(1, width, model), dwk, dwv)

    tok_spec = P(("dp", "tp"))
    return jax.shard_map(
        local_grads,
        mesh=mesh,
        in_specs=(tok_spec, tok_spec, P(None, "tp", None), P(), P(), P("tp")),
        out_specs=(tok_spec, P("dp", "tp", None), tok_spec, tok_spec, tok_spec),
        check_vma=False,
    )
```
